256 devices in a mesh: col: 32 (over z, y), row: 8 (over x, core).
Axes of the slice: x: 4, y: 4, z: 8, core: 2. Of those that a mesh axis runs over, the one named last changes fastest.
Arguments:
- img_emb: bfloat16 [32768, 1024], P(('row', 'col'))
- txt_emb: bfloat16 [32768, 1024], P(('row', 'col'))
- log_scale: float32 [], replicated
Outputs:
- output 1: float32 [], replicated
- output 2: bfloat16 [32768, 1024], P(('row', 'col'))
- output 3: bfloat16 [32768, 1024], P(('row', 'col'))
- output 4: float32 [], replicated
All inputs are finite; a program needn't handle non-finite values.
Results may differ from the reference program's by a relative error of at most 0.001.
Values are sent between devices in bfloat16 or wider.
A program may use at most 768 MiB of HBM per device.

```python
import jax
import jax.numpy as jnp
from jax import lax

ROWS_DEV = 128
SHARDS = 256
EMBED_DIM = 1024
BATCH = ROWS_DEV * SHARDS


def unit_rows(values):
    return values / jnp.sqrt(jnp.sum(values * values, axis=-1, keepdims=True))


def setup_inputs(seed: int = 0) -> dict:
    keys = jax.random.split(jax.random.key(seed), 5)
    shared_dir = unit_rows(jax.random.normal(keys[0], (EMBED_DIM,), jnp.float32))
    spread = (1.0 / EMBED_DIM) ** 0.5
    pair_part = jax.random.normal(keys[1], (BATCH, EMBED_DIM), jnp.float32) * spread
    noise_img = jax.random.normal(keys[2], (BATCH, EMBED_DIM), jnp.float32) * spread
    noise_txt = jax.random.normal(keys[3], (BATCH, EMBED_DIM), jnp.float32) * spread
    img_emb = unit_rows(0.7 * shared_dir + 0.5 * pair_part + 0.5 * noise_img)
    txt_emb = unit_rows(0.7 * shared_dir + 0.5 * pair_part + 0.5 * noise_txt)
    log_scale = jnp.log(jax.random.uniform(keys[4], (), jnp.float32, 10.0, 30.0))
    return {"img_emb": img_emb.astype(jnp.bfloat16), "txt_emb": txt_emb.astype(jnp.bfloat16), "log_scale": log_scale}


def reference(img_emb, txt_emb, log_scale):
    logit_scale = jnp.exp(log_scale)
    img_blocks = img_emb.reshape(SHARDS, ROWS_DEV, EMBED_DIM)
    txt_blocks = txt_emb.reshape(SHARDS, ROWS_DEV, EMBED_DIM)
    block_ids = jnp.arange(SHARDS)
    positions = jnp.arange(BATCH)
    inv_count = 1.0 / (2 * BATCH)

    def row_lse_of(img_block):
        logits = logit_scale * jnp.dot(img_block, txt_emb.T, preferred_element_type=jnp.float32)
        return jax.nn.logsumexp(logits, axis=1)

    def col_lse_of(txt_block):
        logits_t = logit_scale * jnp.dot(txt_block, img_emb.T, preferred_element_type=jnp.float32)
        return jax.nn.logsumexp(logits_t, axis=1)

    row_lse = lax.map(row_lse_of, img_blocks).reshape(BATCH)
    col_lse = lax.map(col_lse_of, txt_blocks).reshape(BATCH)
    pos_logits = logit_scale * jnp.sum(img_emb.astype(jnp.float32) * txt_emb.astype(jnp.float32), axis=1)
    total_loss = (jnp.sum(row_lse - pos_logits) + jnp.sum(col_lse - pos_logits)) * inv_count

    def img_grad_of(block_args):
        block_id, img_block, row_lse_blk = block_args
        logits = logit_scale * jnp.dot(img_block, txt_emb.T, preferred_element_type=jnp.float32)
        diag_mask = (block_id * ROWS_DEV + jnp.arange(ROWS_DEV))[:, None] == positions[None, :]
        grad_tile = (jnp.exp(logits - row_lse_blk[:, None]) + jnp.exp(logits - col_lse[None, :]) - jnp.where(diag_mask, 2.0, 0.0)) * inv_count
        d_block = logit_scale * jnp.dot(grad_tile.astype(jnp.bfloat16), txt_emb, preferred_element_type=jnp.float32)
        return d_block.astype(jnp.bfloat16), jnp.sum(grad_tile * logits)

    def txt_grad_of(block_args):
        block_id, txt_block, col_lse_blk = block_args
        logits_t = logit_scale * jnp.dot(txt_block, img_emb.T, preferred_element_type=jnp.float32)
        diag_mask = (block_id * ROWS_DEV + jnp.arange(ROWS_DEV))[:, None] == positions[None, :]
        grad_t = (jnp.exp(logits_t - row_lse[None, :]) + jnp.exp(logits_t - col_lse_blk[:, None]) - jnp.where(diag_mask, 2.0, 0.0)) * inv_count
        d_block = logit_scale * jnp.dot(grad_t.astype(jnp.bfloat16), img_emb, preferred_element_type=jnp.float32)
        return d_block.astype(jnp.bfloat16)

    d_img, dt_parts = lax.map(img_grad_of, (block_ids, img_blocks, row_lse.reshape(SHARDS, ROWS_DEV)))
    d_txt = lax.map(txt_grad_of, (block_ids, txt_blocks, col_lse.reshape(SHARDS, ROWS_DEV)))
    return total_loss, d_img.reshape(BATCH, EMBED_DIM), d_txt.reshape(BATCH, EMBED_DIM), jnp.sum(dt_parts)
```

```python
import functools

import jax
import jax.numpy as jnp
from jax import lax
from jax.experimental import pallas as pl
from jax.experimental.pallas import tpu as pltpu
from jax.sharding import PartitionSpec as P

MESH = pl.DeviceIdType.MESH
F32 = jnp.float32
BF16 = jnp.bfloat16
W = 128


class Names:
    def __init__(self):
        self.ids = {}

    def __call__(self, *key, count=1):
        if key not in self.ids:
            self.ids[key] = sum(c for _, c in self.ids.values()), count
        return self.ids[key][0]


N_SEM = 224


def kernel(NX, NY, NZ, NC, scale_ref, img_ref, txt_ref, dimg_ref, dtxt_ref, scal_ref,
           iall, tall, imgt, ee, gb, rsum, rel, csum, cel, rall, call_, uref, vref, ub, sc1, sc2,
           recv1, recv2, prt, zrecv, ssem, rsem):
    D = img_ref.shape[1]
    NI, NT = NX * NY, NZ * NC
    XY, ZC = NI > 1, NT > 1
    H, Q = D // 2, D // 4
    inv = 1.0 / (2.0 * W * NI * NT)
    row, col = lax.axis_index("row"), lax.axis_index("col")
    x, c = lax.div(row, NC), lax.rem(row, NC)
    z, y = lax.div(col, NY), lax.rem(col, NY)
    mxy, mzc = x * NY + y, z * NC + c
    scale = scale_ref[0, 0]
    rx = lambda v: lax.rem(v + 2 * NX, NX)
    ry = lambda v: lax.rem(v + 2 * NY, NY)
    rz = lambda v: lax.rem(v + 2 * NZ, NZ)

    def dev(px, py, pz, pc):
        return (pz * NY + py, px * NC + pc)

    plane = [(p, rx(x + p // NY), ry(y + p % NY)) for p in range(1, NI)]
    line = [(p, rz(z + p // NC), lax.rem(c + p % NC, NC)) for p in range(1, NT)]
    barrier = pltpu.get_barrier_semaphore()
    for _, px, py in plane:
        pl.semaphore_signal(barrier, inc=1, device_id=dev(px, py, z, c), device_id_type=MESH)
    for _, pz, pc in line:
        pl.semaphore_signal(barrier, inc=1, device_id=dev(x, y, pz, pc), device_id_type=MESH)
    iall[x, y] = img_ref[...]
    tall[z, c] = txt_ref[...]
    csum[...] = jnp.zeros_like(csum)
    cel[...] = jnp.zeros_like(cel)
    pl.semaphore_wait(barrier, len(plane) + len(line))

    rid, sid = Names(), Names()
    sends = []

    def send(src, dst, key, device, dyn=None):
        n = rid(*key) if dyn is None else rid(key[0], count=16) + dyn
        copy = pltpu.make_async_remote_copy(
            src_ref=src, dst_ref=dst, send_sem=ssem.at[sid(*key)], recv_sem=rsem.at[n],
            device_id=device, device_id_type=MESH)
        copy.start()
        sends.append(copy)

    def got(dst, key, dyn=None):
        n = rid(*key) if dyn is None else rid(key[0], count=16) + dyn
        pltpu.make_async_remote_copy(
            src_ref=dst, dst_ref=dst, send_sem=ssem.at[0], recv_sem=rsem.at[n],
            device_id=dev(x, y, z, c), device_id_type=MESH).wait_recv()

    sg = (1, -1)
    lo, full = W // 4, W // 2

    def rows(half, part=None):
        start, size = half * full, full
        if part is not None:
            start, size = start + part * lo, lo
        return pl.ds(start, size)

    def first_dev(half, d):
        return dev(rx(x + sg[d]), y, z, c) if half == 0 else dev(x, ry(y + sg[d]), z, c)

    def second_dev(half, d):
        return dev(x, ry(y + sg[d]), z, c) if half == 0 else dev(rx(x + sg[d]), y, z, c)

    def first_piece(half, off):
        return (rx(x + off), y) if half == 0 else (x, ry(y + off))

    def second_piece(half, off1, off2):
        return (rx(x + off1), ry(y + off2)) if half == 0 else (rx(x + off2), ry(y + off1))

    def ipc(pc, sl):
        return iall.at[pc[0], pc[1], sl]

    def first_send(half, d, t):
        if t == 1:
            ref = img_ref.at[rows(half)]
            send(ref, ipc((x, y), rows(half)), ("f", half, d, 1), first_dev(half, d))
        else:
            ref = ipc(first_piece(half, -sg[d]), rows(half, d))
            send(ref, ref, ("f", half, d, 2), first_dev(half, d))

    def first_got(half, d, t):
        got(ipc(first_piece(half, -sg[d] * t), rows(half) if t == 1 else rows(half, d)), ("f", half, d, t))

    def second_send(half, off, d, t):
        if t == 1:
            ref = ipc(second_piece(half, off, 0), rows(half))
            src = img_ref.at[rows(half)] if off == 0 else ref
            send(src, ref, ("s", half, off, d, 1), second_dev(half, d))
        else:
            ref = ipc(second_piece(half, off, -sg[d]), rows(half, d))
            send(ref, ref, ("s", half, off, d, 2), second_dev(half, d))

    def second_got(half, off, d, t):
        got(ipc(second_piece(half, off, -sg[d] * t), rows(half) if t == 1 else rows(half, d)), ("s", half, off, d, t))

    def t_send(d, t, h):
        ref = tall.at[rz(z - sg[d] * (t - 1)), c, rows(h)]
        src = txt_ref.at[rows(h)] if t == 1 else ref
        send(src, ref, ("t", d, t, h), dev(x, y, rz(z + sg[d]), c))

    def t_got(d, t, h):
        got(tall.at[rz(z - sg[d] * t), c, rows(h)], ("t", d, t, h))

    def t_pass(off):
        ref = tall.at[rz(z + off), c]
        send(txt_ref if off == 0 else ref, ref, ("p", off), dev(x, y, z, 1 - c))

    def t_passed(off):
        got(tall.at[rz(z + off), 1 - c], ("p", off))

    both = (0, 1)
    if XY:
        for half in both:
            for d in both:
                first_send(half, d, 1)
    if ZC:
        for h in both:
            for d in both:
                t_send(d, 1, h)
        t_pass(0)
    if XY:
        for half in both:
            for d in both:
                second_send(half, 0, d, 1)
        for d in both:
            for half in both:
                first_got(half, d, 1)
                first_send(half, d, 2)
        for d in both:
            for half in both:
                for e in both:
                    second_send(half, -sg[d], e, 1)
    if ZC:
        for h in both:
            for d in both:
                t_got(d, 1, h)
                t_send(d, 2, h)
        t_pass(-1)
        t_pass(1)
    if XY:
        for d in both:
            for half in both:
                second_got(half, 0, d, 1)
                second_send(half, 0, d, 2)
        for d in both:
            for half in both:
                first_got(half, d, 2)
        for half in both:
            for d in both:
                second_send(half, 2, d, 1)
    if ZC:
        for h in both:
            for d in both:
                t_got(d, 2, h)
                t_send(d, 3, h)
        t_pass(-2)
        t_pass(2)
    if XY:
        for off in (-1, 1):
            for d in both:
                for half in both:
                    second_got(half, off, d, 1)
                    second_send(half, off, d, 2)
    if ZC:
        for h in both:
            for d in both:
                t_got(d, 3, h)
                if h == d:
                    t_send(d, 4, h)
        t_pass(-3)
        t_pass(3)
    if XY:
        for d in both:
            for half in both:
                second_got(half, 2, d, 1)
                second_send(half, 2, d, 2)
    if ZC:
        for d in both:
            t_got(d, 4, d)
        t_pass(4)
    if XY:
        for off in (0, -1, 1, 2):
            for d in both:
                for half in both:
                    second_got(half, off, d, 2)
    if ZC:
        for off in (0, -1, 1, -2, 2, -3, 3, 4):
            t_passed(off)

    CW = NC * W

    def logits_rows(i, carry):
        lhs = iall[i].reshape(NY * W, D)
        for zz in range(NZ):
            rhs = tall[zz].reshape(CW, D)
            dots = lax.dot_general(lhs, rhs, (((1,), (1,)), ((), ())), preferred_element_type=F32)
            lg = dots * scale
            e = jnp.exp(lg)
            el = e * lg
            ee[i, 0:NY, :, zz * CW:(zz + 1) * CW] = e.reshape(NY, W, CW)
            for ref, val in ((rsum, e), (rel, el)):
                part = val[:, :W]
                for k in range(1, NC):
                    part = part + val[:, k * W:(k + 1) * W]
                part = part.reshape(NY, W, W)
                ref[i] = part if zz == 0 else ref[i] + part
            for ref, val in ((csum, e), (cel, el)):
                ref[:, zz * CW:(zz + 1) * CW] += jnp.sum(val.reshape(NY * W // 8, 8, CW), axis=0)
        return carry

    lax.fori_loop(0, NX, logits_rows, 0)

    for k in range(NI):
        rall[mxy, k:k + 1, :] = jnp.sum(jnp.transpose(rsum[k // NY, k % NY]), axis=0, keepdims=True)
    for k in range(NT):
        call_[mzc, k:k + 1, :] = jnp.sum(csum[:, k * W:(k + 1) * W], axis=0, keepdims=True)

    def share(buf, key, peers, me, to):
        for p in peers:
            send(buf.at[me], buf.at[me], (key, p[0]), to(p), dyn=me)

    def shared(buf, key, peers, slot):
        for p in peers:
            got(buf.at[slot(p)], (key,), dyn=slot(p))
        total = buf[0]
        for k in range(1, len(peers) + 1):
            total = total + buf[k]
        return total

    to_plane = lambda p: dev(p[1], p[2], z, c)
    to_line = lambda p: dev(x, y, p[1], p[2])
    plane_slot = lambda p: p[1] * NY + p[2]
    line_slot = lambda p: p[1] * NC + p[2]
    share(rall, "r", plane, mxy, to_plane)
    share(call_, "c", line, mzc, to_line)
    for k in range(NI):
        tr = jnp.transpose(iall[k // NY, k % NY])
        for d in both:
            imgt[d, :, k * W:(k + 1) * W] = tr[d * H:(d + 1) * H]
    prod = img_ref[...].astype(F32) * txt_ref[...].astype(F32)
    pos = prod[:, :W]
    for k in range(1, D // W):
        pos = pos + prod[:, k * W:(k + 1) * W]
    pos = scale * jnp.sum(pos, axis=0, keepdims=True)
    rtot = shared(rall, "r", plane, plane_slot)
    uref[...] = rtot
    ctot = shared(call_, "c", line, line_slot)
    vref[...] = ctot
    loss = jnp.log(uref[pl.ds(mxy, 1), :]) + jnp.log(vref[pl.ds(mzc, 1), :]) - 2.0 * pos
    u, v = inv / rtot, inv / ctot
    uref[...] = u
    vref[...] = v

    dts = jnp.zeros((8, W), F32)
    for k in range(NT):
        dts = dts + cel[:, k * W:(k + 1) * W] * v[k:k + 1, :]
    for k in range(NI):
        ub[k // NY, k % NY] = jnp.transpose(jnp.broadcast_to(u[k:k + 1, :], (W, W)))

    def grad_rows(i, acc):
        for j in range(NY):
            uu = ub[i, j]
            acc = acc + jnp.sum((uu * rel[i, j]).reshape(W // 8, 8, W), axis=0)
            for k in range(NT):
                sl = slice(k * W, (k + 1) * W)
                gb[i, j, :, sl] = (ee[i, j, :, sl] * (uu + vref[k:k + 1, :])).astype(BF16)
        return acc

    dts = lax.fori_loop(0, NX, grad_rows, dts)
    own = pl.ds(pl.multiple_of(mzc * W, W), W)
    eye = lax.broadcasted_iota(jnp.int32, (W, W), 0) == lax.broadcasted_iota(jnp.int32, (W, W), 1)
    gb[x, y, :, own] = (ee[x, y, :, own] * (ub[x, y] + vref[pl.ds(mzc, 1), :])
                        - jnp.where(eye, 2.0 * inv, 0.0)).astype(BF16)
    dt_part = jnp.sum(dts, axis=0, keepdims=True) - (2.0 * inv) * pos
    line_no = lax.broadcasted_iota(jnp.int32, (8, W), 0)
    sc1[mxy] = jnp.where(line_no == 0, jnp.broadcast_to(loss * inv, (8, W)),
                         jnp.where(line_no == 1, jnp.broadcast_to(dt_part, (8, W)), 0.0))
    share(sc1, "m", plane, mxy, to_plane)

    def unit_t(s):
        def body(d, carry):
            zz = rz(z - (1 - 2 * d) * (s + 1))
            rhs = gb[:, :, :, pl.ds(pl.multiple_of(zz * CW, W), CW)].reshape(NI * W, CW)
            res = jnp.dot(imgt[d], rhs, preferred_element_type=F32)
            for k in range(NC):
                ee[d * 2 + k, :, :, 1024 + s * W:1024 + (s + 1) * W] = res[:, k * W:(k + 1) * W].reshape(4, W, W)
            return carry

        lax.fori_loop(0, 2, body, 0)

    def unit_i(j):
        for first in both:
            def body(d, carry):
                q = first * 2 + d
                step = (1 - 2 * d) * (j + 1)
                lhs = gb[:, ry(y - step)] if first == 0 else gb[rx(x - step)]
                rhs = tall[:, :, :, pl.ds(pl.multiple_of(q * Q, W), Q)].reshape(NT * W, Q)
                res = jnp.dot(lhs.reshape(4 * W, NT * W), rhs, preferred_element_type=F32)
                ee[q, :, :, j * Q:(j + 1) * Q] = res.reshape(4, W, Q)
                return carry

            lax.fori_loop(0, 2, body, 0)

    def sub(n):
        return pl.ds(n * 2, 2)

    def i_dev(q, d, phase):
        along_y = (q < 2) == (phase == 1)
        return dev(x, ry(y + sg[d]), z, c) if along_y else dev(rx(x + sg[d]), y, z, c)

    def i_place(q, d, s):
        return rx(x - sg[d] * (s + 1)) if q < 2 else ry(y - sg[d] * (s + 1))

    def i_step(j):
        for n in both:
            for q in range(4):
                d = q % 2
                mine = ee.at[q, sub(n), :, pl.ds(j * Q, Q)]
                if j == 0:
                    send(mine, recv1.at[q, 0, sub(n)], ("i", q, 0, n), i_dev(q, d, 1))
                    continue
                here = recv1.at[q, j - 1, sub(n)]
                got(here, ("i", q, j - 1, n))
                here[...] += mine[...]
                if j < 3:
                    send(here, recv1.at[q, j, sub(n)], ("i", q, j, n), i_dev(q, d, 1))

    def i_last(s):
        for q in range(4):
            d = q % 2
            mine = recv1.at[q, 2, i_place(q, d, s)]
            if s == 0:
                send(mine, recv2.at[q, 0], ("j", q, 0), i_dev(q, d, 2))
                continue
            here = recv2.at[q, s - 1]
            got(here, ("j", q, s - 1))
            if s < 3:
                here[...] += mine[...]
                send(here, recv2.at[q, s], ("j", q, s), i_dev(q, d, 2))
            else:
                dimg_ref[:, q * Q:(q + 1) * Q] = ((here[...] + mine[...]) * scale).astype(BF16)

    def t_mine(d, s):
        return ee.at[d * 2 + c, :, :, pl.ds(1024 + s * W, W)]

    def t_swap(s):
        for d in both:
            send(ee.at[d * 2 + 1 - c, :, :, pl.ds(1024 + s * W, W)], prt.at[d, s], ("w", d, s), dev(x, y, z, 1 - c))

    def t_step(s):
        for d in both:
            got(prt.at[d, s], ("w", d, s))
            mine = t_mine(d, s)
            mine[...] += prt[d, s]
        for n in both:
            for d in both:
                mine = ee.at[d * 2 + c, sub(n), :, pl.ds(1024 + s * W, W)]
                if s == 0:
                    send(mine, zrecv.at[d, 0, sub(n)], ("z", d, 0, n), dev(x, y, rz(z + sg[d]), c))
                    continue
                here = zrecv.at[d, s - 1, sub(n)]
                got(here, ("z", d, s - 1, n))
                here[...] += mine[...]
                if s < 7:
                    send(here, zrecv.at[d, s, sub(n)], ("z", d, s, n), dev(x, y, rz(z + sg[d]), c))

    def t_out(block):
        for d in both:
            for k in range(4):
                w = d * 4 + k
                dtxt_ref[:, w * W:(w + 1) * W] = (jnp.transpose(block(d, k)) * scale).astype(BF16)

    for s in range(8):
        if ZC:
            unit_t(s)
            t_swap(s)
        if XY and s % 2 == 0:
            unit_i(s // 2)
            i_step(s // 2)
        if XY and s == 6:
            i_last(0)
        if ZC:
            t_step(s)
        if s == 3:
            sc2[mzc] = shared(sc1, "m", plane, plane_slot)
            share(sc2, "n", line, mzc, to_line)
    if XY:
        for s in range(1, 4):
            i_last(s)
    else:
        for q in range(4):
            rhs = tall[:, :, :, q * Q:(q + 1) * Q].reshape(NT * W, Q)
            res = jnp.dot(gb[0, 0], rhs, preferred_element_type=F32)
            dimg_ref[:, q * Q:(q + 1) * Q] = (res * scale).astype(BF16)
    if ZC:
        t_out(lambda d, k: zrecv[d, 6, k])
    else:
        for d in both:
            res = jnp.dot(imgt[d], gb[...].reshape(NI * W, W), preferred_element_type=F32)
            for k in range(4):
                w = d * 4 + k
                dtxt_ref[:, w * W:(w + 1) * W] = (jnp.transpose(res[k * W:(k + 1) * W]) * scale).astype(BF16)
    total = shared(sc2, "n", line, line_slot)
    scal_ref[...] = jnp.broadcast_to(jnp.sum(total, axis=1, keepdims=True), (8, W))
    for copy in sends:
        copy.wait_send()


def call(NX, NY, NZ, NC, scale, img, txt):
    D = img.shape[1]
    NI, NT = NX * NY, NZ * NC
    H, Q = D // 2, D // 4
    vmem = pltpu.VMEM
    return pl.pallas_call(
        functools.partial(kernel, NX, NY, NZ, NC),
        out_shape=(jax.ShapeDtypeStruct(img.shape, BF16), jax.ShapeDtypeStruct(txt.shape, BF16),
                   jax.ShapeDtypeStruct((8, W), F32)),
        in_specs=[pl.BlockSpec(memory_space=pltpu.SMEM)] + [pl.BlockSpec(memory_space=vmem)] * 2,
        out_specs=[pl.BlockSpec(memory_space=vmem)] * 3,
        scratch_shapes=[
            vmem((NX, NY, W, D), BF16), vmem((NZ, NC, W, D), BF16), vmem((2, H, NI * W), BF16),
            vmem((4, 4, W, 2048), F32), vmem((NX, NY, W, NT * W), BF16),
            vmem((NX, NY, W, W), F32), vmem((NX, NY, W, W), F32), vmem((8, NT * W), F32), vmem((8, NT * W), F32),
            vmem((NI, NI, W), F32), vmem((NT, NT, W), F32), vmem((NI, W), F32), vmem((NT, W), F32),
            vmem((NX, NY, W, W), F32), vmem((NI, 8, W), F32), vmem((NT, 8, W), F32),
            vmem((4, 3, 4, W, Q), F32), vmem((4, 3, W, Q), F32),
            vmem((2, 8, 4, W, W), F32), vmem((2, 7, 4, W, W), F32),
            pltpu.SemaphoreType.DMA((N_SEM,)), pltpu.SemaphoreType.DMA((N_SEM,)),
        ],
        compiler_params=pltpu.CompilerParams(collective_id=0, has_side_effects=True, vmem_limit_bytes=67043328),
    )(scale, img, txt)


SHAPE = (4, 4, 8, 2)


def solution(mesh):
    batch_spec = P(("row", "col"), None)

    def local_tile(img_loc, txt_loc, log_scale):
        scale = jnp.exp(log_scale).reshape(1, 1)
        d_img, d_txt, scal = call(*SHAPE, scale, img_loc, txt_loc)
        return scal[0, 0], d_img, d_txt, scal[1, 0]

    return jax.shard_map(local_tile, mesh=mesh, in_specs=(batch_spec, batch_spec, P()),
                         out_specs=(P(), batch_spec, batch_spec, P()), check_vma=False)
```

```python
import functools

import jax
import jax.numpy as jnp
from jax import lax
from jax.experimental import pallas as pl
from jax.experimental.pallas import tpu as pltpu
from jax.sharding import PartitionSpec as P

MESH = pl.DeviceIdType.MESH
F32 = jnp.float32
LOG2E = 1.4426950408889634
BF16 = jnp.bfloat16
W = 128


N_SEND, N_RECV = 14, 198


class Names:
    def __init__(self):
        self.ids = {}

    def __call__(self, *key):
        return self.ids.setdefault(key, len(self.ids))


def block_of(tiles):
    for a in range(1, 5):
        for b in range(1, 5):
            for r in range(1, 17):
                if tiles % (a * b * r) == 0 and tiles // (a * b * r) <= 16:
                    return a, b, r * 8, tiles // (a * b * r) * 128
    raise ValueError(tiles)


def kernel(NX, NY, NZ, NC, scale_ref, img_ref, txt_ref, dimg_ref, dtxt_ref, scal_ref,
           iall, tall, imgt, ee, gb, rsum, rel, csum, cel, rall, call_, uref, vref, ub, sc1, sc2,
           recv1, recv2, prt, zrecv, lead, ssem, rsem):
    D = img_ref.shape[1]
    NI, NT = NX * NY, NZ * NC
    XY, ZC = NI > 1, NT > 1
    H, Q = D // 2, D // 4
    inv = 1.0 / (2.0 * W * NI * NT)
    row, col = lax.axis_index("row"), lax.axis_index("col")
    x, c = lax.div(row, NC), lax.rem(row, NC)
    z, y = lax.div(col, NY), lax.rem(col, NY)
    mxy, mzc = x * NY + y, z * NC + c
    scale = scale_ref[0, 0]
    scale2 = scale * LOG2E
    rx = lambda v: lax.rem(v + 2 * NX, NX)
    ry = lambda v: lax.rem(v + 2 * NY, NY)
    rz = lambda v: lax.rem(v + 2 * NZ, NZ)

    def dev(px, py, pz, pc):
        return (pz * NY + py, px * NC + pc)

    plane = [(p, rx(x + p // NY), ry(y + p % NY)) for p in range(1, NI)]
    line = [(p, rz(z + p // NC), lax.rem(c + p % NC, NC)) for p in range(1, NT)]
    barrier = pltpu.get_barrier_semaphore()
    greet = []
    if XY:
        greet += [dev(rx(x + k), y, z, c) for k in (1, -1)] + [dev(x, ry(y + k), z, c) for k in (1, -1)]
    if ZC:
        greet += [dev(x, y, rz(z + k), c) for k in (1, -1)] + [dev(x, y, z, 1 - c)]
    for device in greet:
        pl.semaphore_signal(barrier, inc=1, device_id=device, device_id_type=MESH)
    iall[x, y] = img_ref[...]
    tall[z, c] = txt_ref[...]
    for ref in (csum, cel, rsum, rel):
        ref[...] = jnp.zeros_like(ref)
    with jax.named_scope("barrier"):
        pl.semaphore_wait(barrier, len(greet))

    rid, sid = Names(), Names()
    sent = {}
    times = [1]

    def send(src, dst, key, device, group, offset=0):
        pltpu.make_async_remote_copy(
            src_ref=src, dst_ref=dst, send_sem=ssem.at[sid(group)], recv_sem=rsem.at[rid(*key) + offset],
            device_id=device, device_id_type=MESH).start()
        size = jnp.dtype(src.dtype).itemsize
        for n in src.shape:
            size *= n
        sent[group] = sent.get(group, 0) + size * times[0]

    def got(dst, key):
        pltpu.make_async_remote_copy(
            src_ref=dst, dst_ref=dst, send_sem=ssem.at[0], recv_sem=rsem.at[rid(*key)],
            device_id=dev(x, y, z, c), device_id_type=MESH).wait_recv()

    sg = (1, -1)
    lo, full = W // 4, W // 2

    def rows(half, part=None):
        start, size = half * full, full
        if part is not None:
            start, size = start + part * lo, lo
        return pl.ds(start, size)

    def first_dev(half, d):
        return dev(rx(x + sg[d]), y, z, c) if half == 0 else dev(x, ry(y + sg[d]), z, c)

    def second_dev(half, d):
        return dev(x, ry(y + sg[d]), z, c) if half == 0 else dev(rx(x + sg[d]), y, z, c)

    def first_piece(half, off):
        return (rx(x + off), y) if half == 0 else (x, ry(y + off))

    def second_piece(half, off1, off2):
        return (rx(x + off1), ry(y + off2)) if half == 0 else (rx(x + off2), ry(y + off1))

    def ipc(pc, sl):
        return iall.at[pc[0], pc[1], sl]

    def first_send(half, d, t):
        if t == 1:
            ref = img_ref.at[rows(half)]
            send(ref, ipc((x, y), rows(half)), ("f", half, d, 1), first_dev(half, d), "f1")
        else:
            ref = ipc(first_piece(half, -sg[d]), rows(half, d))
            send(ref, ref, ("f", half, d, 2), first_dev(half, d), "f2")

    def first_got(half, d, t):
        got(ipc(first_piece(half, -sg[d] * t), rows(half) if t == 1 else rows(half, d)), ("f", half, d, t))

    def second_send(half, off, d, t):
        if t == 1:
            ref = ipc(second_piece(half, off, 0), rows(half))
            src = img_ref.at[rows(half)] if off == 0 else ref
            send(src, ref, ("s", half, off, d, 1), second_dev(half, d), "s1")
        else:
            ref = ipc(second_piece(half, off, -sg[d]), rows(half, d))
            send(ref, ref, ("s", half, off, d, 2), second_dev(half, d), "s2")

    def second_got(half, off, d, t):
        got(ipc(second_piece(half, off, -sg[d] * t), rows(half) if t == 1 else rows(half, d)), ("s", half, off, d, t))

    def t_send(d, t, h):
        ref = tall.at[rz(z - sg[d] * (t - 1)), c, rows(h)]
        src = txt_ref.at[rows(h)] if t == 1 else ref
        send(src, ref, ("t", d, t, h), dev(x, y, rz(z + sg[d]), c), "t")

    def t_got(d, t, h):
        got(tall.at[rz(z - sg[d] * t), c, rows(h)], ("t", d, t, h))

    def t_pass(off):
        if ZC:
            ref = tall.at[rz(z + off), c]
            send(txt_ref if off == 0 else ref, ref, ("p", off), dev(x, y, z, 1 - c), "p")

    def t_passed(*offs):
        if ZC:
            for off in offs:
                got(tall.at[rz(z + off), 1 - c], ("p", off))

    both = (0, 1)

    def t_round(t):
        if ZC:
            for h in both:
                for d in both:
                    t_got(d, t, h)
                    if t < 3 or h == d:
                        t_send(d, t + 1, h)
            t_pass(-t)
            t_pass(t)

    def s_round(offs, t, halves=both):
        if XY:
            for off in offs:
                for d in both:
                    for half in halves:
                        second_got(half, off, d, t)
                        if t == 1:
                            second_send(half, off, d, 2)

    CW = NC * W

    def logits(shards, zs):
        lhs = jnp.concatenate([iall[i, j] for i, j in shards], axis=0)
        for zz in zs:
            cols = pl.ds(pl.multiple_of(zz * CW, W), CW)
            rhs = tall[zz].reshape(CW, D)
            dots = lax.dot_general(lhs, rhs, (((1,), (1,)), ((), ())), preferred_element_type=F32)
            lg = dots * scale2
            e = jnp.exp2(lg)
            el = e * lg
            for n, (i, j) in enumerate(shards):
                ee[i, j, :, cols] = e[n * W:(n + 1) * W]
            for ref, val in ((rsum, e), (rel, el)):
                part = val[:, :W]
                for k in range(1, NC):
                    part = part + val[:, k * W:(k + 1) * W]
                for n, (i, j) in enumerate(shards):
                    ref[i, j] += part[n * W:(n + 1) * W]
            for ref, val in ((csum, e), (cel, el)):
                ref[:, cols] += jnp.sum(val.reshape(len(shards) * W // 8, 8, CW), axis=0)

    def near(name, *offs):
        with jax.named_scope(name):
            zs = [rz(z + off) for off in offs] if ZC else [z] if 0 in offs else []
            if not zs:
                return
            if not XY:
                logits([(x, y)], zs)
                return

            def body(g, carry):
                i = rx(x + g - 1)
                logits([(i, ry(y - 1)), (i, y), (i, ry(y + 1))], zs)
                return carry

            lax.fori_loop(0, 3, body, 0)

    def across(name, *offs):
        with jax.named_scope(name):
            zs = [rz(z + off) for off in offs] if ZC else [z] if 0 in offs else []
            if XY and zs:
                logits([(x, ry(y + 2)), (rx(x + 2), y)], zs)

    def far(name):
        with jax.named_scope(name):
            if not XY:
                return
            shards = [(rx(x - 1), ry(y + 2)), (rx(x + 1), ry(y + 2))] + [(rx(x + 2), ry(y + k)) for k in (-1, 1, 2)]
            if not ZC:
                logits(shards, [z])
                return

            def body(p, carry):
                logits(shards, [rz(z - p), rz(z + jnp.where(p == 0, 4, p))])
                return carry

            lax.fori_loop(0, 4, body, 0)

    if XY:
        for half in both:
            for d in both:
                first_send(half, d, 1)
    if ZC:
        for h in both:
            for d in both:
                t_send(d, 1, h)
        t_pass(0)
    if XY:
        for half in both:
            for d in both:
                second_send(half, 0, d, 1)
        with jax.named_scope("f1"):
            for d in both:
                for half in both:
                    first_got(half, d, 1)
                    first_send(half, d, 2)
        for d in both:
            for half in both:
                for e in both:
                    second_send(half, -sg[d], e, 1)
    with jax.named_scope("T1"):
        t_round(1)
    with jax.named_scope("s0"):
        s_round((0,), 1)
    if XY:
        with jax.named_scope("f2"):
            for d in both:
                for half in both:
                    first_got(half, d, 2)
        for half in both:
            for d in both:
                second_send(half, 2, d, 1)
    with jax.named_scope("s1"):
        s_round((-1, 1), 1)
    with jax.named_scope("T2"):
        t_round(2)
    with jax.named_scope("p1"):
        t_passed(0, -1, 1)
    near("C1", -1, 0, 1)
    with jax.named_scope("p2"):
        t_passed(-2, 2)
    near("C2", -2, 2)
    with jax.named_scope("s2"):
        s_round((2,), 1)
    with jax.named_scope("s0t2"):
        s_round((0,), 2)
    across("C3", -2, -1, 0, 1, 2)
    with jax.named_scope("T3"):
        t_round(3)
    with jax.named_scope("p3"):
        t_passed(-3, 3)
    near("C4", -3, 3)
    with jax.named_scope("T4"):
        if ZC:
            for d in both:
                t_got(d, 4, d)
            t_pass(4)
    across("C4b", -3, 3)
    with jax.named_scope("p4"):
        t_passed(4)
    near("C5", 4)
    across("C5b", 4)
    with jax.named_scope("end"):
        s_round((-1, 1), 2)
        s_round((2,), 2)
    far("C6")

    for k in range(NI):
        rall[mxy, k:k + 1, :] = jnp.sum(jnp.transpose(rsum[k // NY, k % NY]), axis=0, keepdims=True)
    for k in range(NT):
        call_[mzc, k:k + 1, :] = jnp.sum(csum[:, k * W:(k + 1) * W], axis=0, keepdims=True)

    def share(buf, key, peers, me, to):
        for p in peers:
            send(buf.at[me], buf.at[me], (key,), to(p), key)

    def shared(buf, key, peers):
        if peers:
            got(buf.at[pl.ds(0, len(peers))], (key,))
        total = buf[0]
        for k in range(1, len(peers) + 1):
            total = total + buf[k]
        return total

    to_plane = lambda p: dev(p[1], p[2], z, c)
    to_line = lambda p: dev(x, y, p[1], p[2])
    share(rall, "r", plane, mxy, to_plane)
    share(call_, "c", line, mzc, to_line)
    with jax.named_scope("imgt"):
        for k in range(NI):
            tr = jnp.transpose(iall[k // NY, k % NY])
            for d in both:
                imgt[d, :, k * W:(k + 1) * W] = tr[d * H:(d + 1) * H]
        prod = img_ref[...].astype(F32) * txt_ref[...].astype(F32)
        pos = prod[:, :W]
        for k in range(1, D // W):
            pos = pos + prod[:, k * W:(k + 1) * W]
        pos = scale * jnp.sum(pos, axis=0, keepdims=True)
    with jax.named_scope("rwait"):
        rtot = shared(rall, "r", plane)
    u = inv / rtot
    for k in range(NI):
        ub[k // NY, k % NY] = jnp.transpose(jnp.broadcast_to(u[k:k + 1, :], (W, W)))
    with jax.named_scope("cwait"):
        ctot = shared(call_, "c", line)
    v = inv / ctot
    uref[...] = rtot
    vref[...] = v

    def build(i, j):
        uu = ub[i, j]
        for k in range(NT):
            sl = slice(k * W, (k + 1) * W)
            gb[i, j, :, sl] = (ee[i, j, :, sl] * (uu + vref[k:k + 1, :])).astype(BF16)

    def builds(n, place):
        def body(k, carry):
            build(*place(k))
            return carry

        lax.fori_loop(0, n, body, 0)

    for q in range(4):
        for k in range(4):
            rid("i", q, 0, k)
    for s in range(8):
        for d in both:
            rid("w", s, d)

    def unit_t(s):
        def body(d, carry):
            zz = rz(z - (1 - 2 * d) * (s + 1))
            rhs = gb[:, :, :, pl.ds(pl.multiple_of(zz * CW, W), CW)].reshape(NI * W, CW)
            res = jnp.dot(imgt[d], rhs, preferred_element_type=F32)
            for k in range(NC):
                ee[d * 2 + k, :, :, 1024 + s * W:1024 + (s + 1) * W] = res[:, k * W:(k + 1) * W].reshape(4, W, W)
            send(ee.at[d * 2 + 1 - c, :, :, pl.ds(1024 + s * W, W)], prt.at[d, s], ("w", s, 0), dev(x, y, z, 1 - c), "w", d)
            return carry

        with jax.named_scope(f"ut{s}"):
            times[0] = 2
            lax.fori_loop(0, 2, body, 0)
            times[0] = 1

    def unit_i1(first, d, j):
        q = first * 2 + d
        step = (1 - 2 * d) * (j + 1)
        lhs = gb[:, ry(y - step)] if first == 0 else gb[rx(x - step)]
        rhs = tall[:, :, :, pl.ds(pl.multiple_of(q * Q, W), Q)].reshape(NT * W, Q)
        res = jnp.dot(lhs.reshape(4 * W, NT * W), rhs, preferred_element_type=F32)
        if j == 0:
            lead[q] = res.reshape(4, W, Q)
        else:
            ee[q, :, :, j * Q:(j + 1) * Q] = res.reshape(4, W, Q)

    def unit_i(first, j):
        def body(d, carry):
            unit_i1(first, d, j)
            return carry

        with jax.named_scope(f"ui{first}{j}"):
            lax.fori_loop(0, 2, body, 0)

    def i_dev(q, phase):
        d = q % 2
        along_y = (q < 2) == (phase == 1)
        return dev(x, ry(y + sg[d]), z, c) if along_y else dev(rx(x + sg[d]), y, z, c)

    def i_place(q, k):
        d = q % 2
        return rx(x - sg[d] * (k + 1)) if q < 2 else ry(y - sg[d] * (k + 1))

    def i_step(q, j, k):
        at = i_place(q, k)
        mine = ee.at[q, at, :, pl.ds(j * Q, Q)]
        here = recv1.at[q, j - 1, at]
        got(here, ("i", q, j - 1, k))
        here[...] += mine[...]
        if j < 3:
            send(here, recv1.at[q, j, at], ("i", q, j, k), i_dev(q, 1), "i")
        elif k == 0:
            send(here, recv2.at[q, 0], ("j", q, 0), i_dev(q, 2), "j")

    def i_last(q, s):
        mine = recv1.at[q, 2, i_place(q, s)]
        here = recv2.at[q, s - 1]
        got(here, ("j", q, s - 1))
        if s < 3:
            here[...] += mine[...]
            send(here, recv2.at[q, s], ("j", q, s), i_dev(q, 2), "j")
        else:
            dimg_ref[:, q * Q:(q + 1) * Q] = ((here[...] + mine[...]) * scale).astype(BF16)

    def z_step(d, s, k):
        if k == 0:
            got(prt.at[d, s], ("w", s, d))
        mine = ee.at[d * 2 + c, k, :, pl.ds(1024 + s * W, W)]
        if s == 0:
            mine[...] += prt[d, s, k]
            here = mine
        else:
            here = zrecv.at[d, s - 1, k]
            got(here, ("z", d, s - 1, k))
        if s == 7:
            w = d * 4 + k
            block = here[...] + (mine[...] + prt[d, s, k])
            dtxt_ref[:, w * W:(w + 1) * W] = (jnp.transpose(block) * scale).astype(BF16)
            return
        if s > 0:
            here[...] += mine[...] + prt[d, s, k]
        send(here, zrecv.at[d, s, k], ("z", d, s, k), dev(x, y, rz(z + sg[d]), c), "z")

    def totals():
        dts = jnp.zeros((8, W), F32)
        for k in range(NT):
            dts = dts + cel[:, k * W:(k + 1) * W] * vref[k:k + 1, :]

        def body(i, acc):
            for j in range(NY):
                acc = acc + jnp.sum((ub[i, j] * rel[i, j]).reshape(W // 8, 8, W), axis=0)
            return acc

        dts = lax.fori_loop(0, NX, body, dts)
        dt_part = jnp.sum(dts, axis=0, keepdims=True) * (1.0 / LOG2E) - (2.0 * inv) * pos
        loss = jnp.log(uref[pl.ds(mxy, 1), :]) - jnp.log(vref[pl.ds(mzc, 1), :] * (1.0 / inv)) - 2.0 * pos
        line_no = lax.broadcasted_iota(jnp.int32, (8, W), 0)
        sc1[mxy] = jnp.where(line_no == 0, jnp.broadcast_to(loss * inv, (8, W)),
                             jnp.where(line_no == 1, jnp.broadcast_to(dt_part, (8, W)), 0.0))
        share(sc1, "m", plane, mxy, to_plane)

    def totals2():
        sc2[mzc] = shared(sc1, "m", plane)
        share(sc2, "n", line, mzc, to_line)

    def start(d, carry):
        sign = 1 - 2 * d
        builds(4 - d, lambda k: (rx(x + k), ry(y - sign)))
        unit_i1(0, d, 0)
        for k in range(4):
            at = rx(x - sign * (k + 1))
            send(lead.at[d, at], recv1.at[d, 0, at], ("i", 0, 0, k), dev(x, ry(y + sign), z, c), "i", 4 * d)
        builds(3 - d, lambda k: (rx(x - sign), ry(y + k * (1 + d))))
        unit_i1(1, d, 0)
        for k in range(4):
            at = ry(y - sign * (k + 1))
            send(lead.at[2 + d, at], recv1.at[2 + d, 0, at], ("i", 2, 0, k), dev(rx(x + sign), y, z, c), "i", 4 * d)
        return carry

    if XY:
        with jax.named_scope("start"):
            times[0] = 2
            lax.fori_loop(0, 2, start, 0)
            times[0] = 1
        builds(4, lambda k: (rx(x + 2 * lax.div(k, 2)), ry(y + 2 * lax.rem(k, 2))))
    else:
        build(0, 0)
    own = pl.ds(pl.multiple_of(mzc * W, W), W)
    eye = lax.broadcasted_iota(jnp.int32, (W, W), 0) == lax.broadcasted_iota(jnp.int32, (W, W), 1)
    gb[x, y, :, own] = (ee[x, y, :, own] * (ub[x, y] + vref[pl.ds(mzc, 1), :])
                        - jnp.where(eye, 2.0 * inv, 0.0)).astype(BF16)
    if ZC:
        unit_t(0)

    PERIOD, LAT = 11.3, 2.0
    base = {0: 0.0, 2: 1.2, 1: 2.4, 3: 3.5}
    zbase = 6.5
    events, work = [], []
    if ZC:
        for k in range(4):
            for d in both:
                events.append((zbase + 0.01 * k, 1, ("z", d, 0, k)))
        for s in range(1, 8):
            t0 = zbase + (s - 1) * PERIOD / 2 + LAT
            work.append((t0 + PERIOD / 8, ("ut", s)))
            for k in range(4):
                for d in both:
                    events.append((t0 + (k + 1) * PERIOD / 8, 1, ("z", d, s, k)))
    if XY:
        for q in range(4):
            for j in range(1, 4):
                t0 = base[q] + (j - 1) * PERIOD + LAT + 2.5
                if q % 2 == 0:
                    work.append((t0 + PERIOD / 4, ("ui", q // 2, j)))
                for k in range(4):
                    t = t0 + (k + 1) * PERIOD / 4
                    events.append((t, 2, ("i", q, j, k)))
                    if j == 3 and k:
                        events.append((max(t, base[q] + 32.0 + 4.8 * k), 3, ("j", q, k)))
    events.append((zbase + 3.0, 0, ("totals",)))
    events.append((zbase + 20.0, 0, ("totals2",)))
    events.sort()
    work.sort()
    needs = {}
    for t, what in work:
        if what[0] == "ut":
            needs[what] = lambda e, s=what[1]: e[0] == "z" and e[2] == s
        else:
            needs[what] = lambda e, f=what[1], j=what[2]: e[0] == "i" and e[1] // 2 == f and e[2] == j
    now = 5.5
    run = {"z": z_step, "i": i_step, "j": i_last, "totals": totals, "totals2": totals2, "ut": unit_t, "ui": unit_i}
    for t, _, event in events:
        while work and (now + 1.5 <= t + 0.3 or any(needs[w](event) for _, w in work)):
            _, w = work.pop(0)
            run[w[0]](*w[1:])
            now += 1.5
        with jax.named_scope("_".join(str(v) for v in event)):
            run[event[0]](*event[1:])
        now = max(now, t) + 0.07

    if not XY:
        for q in range(4):
            rhs = tall[:, :, :, q * Q:(q + 1) * Q].reshape(NT * W, Q)
            res = jnp.dot(gb[0, 0], rhs, preferred_element_type=F32)
            dimg_ref[:, q * Q:(q + 1) * Q] = (res * scale).astype(BF16)
    if not ZC:
        for d in both:
            res = jnp.dot(imgt[d], gb[...].reshape(NI * W, W), preferred_element_type=F32)
            for k in range(4):
                w = d * 4 + k
                dtxt_ref[:, w * W:(w + 1) * W] = (jnp.transpose(res[k * W:(k + 1) * W]) * scale).astype(BF16)
    with jax.named_scope("fin"):
        total = shared(sc2, "n", line)
        scal_ref[...] = jnp.broadcast_to(jnp.sum(total, axis=1, keepdims=True), (8, W))
    for group, size in sent.items():
        a, b, r, l = block_of(size // 4096)
        ref = ee.at[pl.ds(0, a), pl.ds(0, b), pl.ds(0, r), pl.ds(0, l)]
        pltpu.make_async_remote_copy(
            src_ref=ref, dst_ref=ref, send_sem=ssem.at[sid(group)], recv_sem=rsem.at[0],
            device_id=dev(x, y, z, c), device_id_type=MESH).wait_send()
    assert len(sid.ids) <= N_SEND and len(rid.ids) <= N_RECV, (len(sid.ids), len(rid.ids))

def call(NX, NY, NZ, NC, scale, img, txt):
    D = img.shape[1]
    NI, NT = NX * NY, NZ * NC
    H, Q = D // 2, D // 4
    vmem = pltpu.VMEM
    return pl.pallas_call(
        functools.partial(kernel, NX, NY, NZ, NC),
        out_shape=(jax.ShapeDtypeStruct(img.shape, BF16), jax.ShapeDtypeStruct(txt.shape, BF16),
                   jax.ShapeDtypeStruct((8, W), F32)),
        in_specs=[pl.BlockSpec(memory_space=pltpu.SMEM)] + [pl.BlockSpec(memory_space=vmem)] * 2,
        out_specs=[pl.BlockSpec(memory_space=vmem)] * 3,
        scratch_shapes=[
            vmem((NX, NY, W, D), BF16), vmem((NZ, NC, W, D), BF16), vmem((2, H, NI * W), BF16),
            vmem((4, 4, W, 2048), F32), vmem((NX, NY, W, NT * W), BF16),
            vmem((NX, NY, W, W), F32), vmem((NX, NY, W, W), F32), vmem((8, NT * W), F32), vmem((8, NT * W), F32),
            vmem((NI, NI, W), F32), vmem((NT, NT, W), F32), vmem((NI, W), F32), vmem((NT, W), F32),
            vmem((NX, NY, W, W), F32), vmem((NI, 8, W), F32), vmem((NT, 8, W), F32),
            vmem((4, 3, 4, W, Q), F32), vmem((4, 3, W, Q), F32),
            vmem((2, 8, 4, W, W), F32), vmem((2, 7, 4, W, W), F32), vmem((4, 4, W, Q), F32),
            pltpu.SemaphoreType.DMA((N_SEND,)), pltpu.SemaphoreType.DMA((N_RECV,)),
        ],
        compiler_params=pltpu.CompilerParams(collective_id=0, has_side_effects=True, vmem_limit_bytes=67043328),
    )(scale, img, txt)


SHAPE = (4, 4, 8, 2)


def solution(mesh):
    batch_spec = P(("row", "col"), None)

    def local_tile(img_loc, txt_loc, log_scale):
        scale = jnp.exp(log_scale).reshape(1, 1)
        d_img, d_txt, scal = call(*SHAPE, scale, img_loc, txt_loc)
        return scal[0, 0], d_img, d_txt, scal[1, 0]

    return jax.shard_map(local_tile, mesh=mesh, in_specs=(batch_spec, batch_spec, P()),
                         out_specs=(P(), batch_spec, batch_spec, P()), check_vma=False)
```

```python
import functools

import jax
import jax.numpy as jnp
from jax import lax
from jax.experimental import pallas as pl
from jax.experimental.pallas import tpu as pltpu
from jax.sharding import PartitionSpec as P

MESH = pl.DeviceIdType.MESH
F32 = jnp.float32
LOG2E = 1.4426950408889634
BF16 = jnp.bfloat16
W = 128


N_SEND, N_RECV = 14, 98


class Names:
    def __init__(self):
        self.ids = {}

    def __call__(self, *key):
        return self.ids.setdefault(key, len(self.ids))


def block_of(tiles):
    for a in range(1, 5):
        for b in range(1, 5):
            for r in range(1, 17):
                if tiles % (a * b * r) == 0 and tiles // (a * b * r) <= 16:
                    return a, b, r * 8, tiles // (a * b * r) * 128
    raise ValueError(tiles)


def kernel(NX, NY, NZ, NC, scale_ref, img_ref, txt_ref, dimg_ref, dtxt_ref, scal_ref,
           iall, tall, imgt, ee, gb, rsum, rel, csum, cel, rall, call_, uref, vref, ub, sc1, sc2,
           recv1, recv2, prt, zrecv, lead, ssem, rsem, lsem):
    D = img_ref.shape[1]
    NI, NT = NX * NY, NZ * NC
    XY, ZC = NI > 1, NT > 1
    H, Q = D // 2, D // 4
    inv = 1.0 / (2.0 * W * NI * NT)
    row, col = lax.axis_index("row"), lax.axis_index("col")
    x, c = lax.div(row, NC), lax.rem(row, NC)
    z, y = lax.div(col, NY), lax.rem(col, NY)
    mxy, mzc = x * NY + y, z * NC + c
    scale = scale_ref[0, 0]
    scale2 = scale * LOG2E
    rx = lambda v: lax.rem(v + 2 * NX, NX)
    ry = lambda v: lax.rem(v + 2 * NY, NY)
    rz = lambda v: lax.rem(v + 2 * NZ, NZ)

    def dev(px, py, pz, pc):
        return (pz * NY + py, px * NC + pc)

    plane = [(p, rx(x + p // NY), ry(y + p % NY)) for p in range(1, NI)]
    line = [(p, rz(z + p // NC), lax.rem(c + p % NC, NC)) for p in range(1, NT)]
    barrier = pltpu.get_barrier_semaphore()
    greet = []
    if XY:
        greet += [dev(rx(x + k), y, z, c) for k in (1, -1)] + [dev(x, ry(y + k), z, c) for k in (1, -1)]
    if ZC:
        greet += [dev(x, y, rz(z + k), c) for k in (1, -1)] + [dev(x, y, z, 1 - c)]
    for device in greet:
        pl.semaphore_signal(barrier, inc=1, device_id=device, device_id_type=MESH)
    loads = [pltpu.make_async_copy(img_ref, iall.at[x, y], lsem.at[0]), pltpu.make_async_copy(txt_ref, tall.at[z, c], lsem.at[1])]
    for load in loads:
        load.start()
    for ref in (csum, cel, rsum, rel, sc1, sc2):
        ref[...] = jnp.zeros_like(ref)
    with jax.named_scope("barrier"):
        for load in loads:
            load.wait()
        pl.semaphore_wait(barrier, len(greet))

    rid, sid = Names(), Names()
    sent = {}
    times = [1]

    def send(src, dst, key, device, group, offset=0):
        pltpu.make_async_remote_copy(
            src_ref=src, dst_ref=dst, send_sem=ssem.at[sid(group)], recv_sem=rsem.at[rid(*key) + offset],
            device_id=device, device_id_type=MESH).start()
        size = jnp.dtype(src.dtype).itemsize
        for n in src.shape:
            size *= n
        sent[group] = sent.get(group, 0) + size * times[0]

    def got(dst, key):
        pltpu.make_async_remote_copy(
            src_ref=dst, dst_ref=dst, send_sem=ssem.at[0], recv_sem=rsem.at[rid(*key)],
            device_id=dev(x, y, z, c), device_id_type=MESH).wait_recv()

    sg = (1, -1)
    lo, full = W // 4, W // 2

    def rows(half, part=None):
        start, size = half * full, full
        if part is not None:
            start, size = start + part * lo, lo
        return pl.ds(start, size)

    def first_dev(half, d):
        return dev(rx(x + sg[d]), y, z, c) if half == 0 else dev(x, ry(y + sg[d]), z, c)

    def second_dev(half, d):
        return dev(x, ry(y + sg[d]), z, c) if half == 0 else dev(rx(x + sg[d]), y, z, c)

    def first_piece(half, off):
        return (rx(x + off), y) if half == 0 else (x, ry(y + off))

    def second_piece(half, off1, off2):
        return (rx(x + off1), ry(y + off2)) if half == 0 else (rx(x + off2), ry(y + off1))

    def ipc(pc, sl):
        return iall.at[pc[0], pc[1], sl]

    def got_images(shards, key):
        got(iall.at[0, pl.ds(0, shards)], key)

    def got_texts(shards, key):
        got(tall.at[pl.ds(0, shards), 0], key)

    def first_send(half, d, t):
        if t == 1:
            ref = ipc((x, y), rows(half))
            send(ref, ref, ("f", d), first_dev(half, d), "f1")
        else:
            ref = ipc(first_piece(half, -sg[d]), rows(half, d))
            send(ref, ref, ("f2",), first_dev(half, d), "f2")

    def second_send(half, off, d, t):
        if t == 1:
            ref = ipc(second_piece(half, off, 0), rows(half))
            send(ref, ref, ("s", abs(off), d), second_dev(half, d), "s1")
        else:
            ref = ipc(second_piece(half, off, -sg[d]), rows(half, d))
            send(ref, ref, ("s2", off == 0), second_dev(half, d), "s2")

    def t_send(d, t, h):
        ref = tall.at[rz(z - sg[d] * (t - 1)), c, rows(h)]
        send(ref, ref, ("t", t, h if t < 4 else 0), dev(x, y, rz(z + sg[d]), c), "t")

    def t_pass(off):
        if ZC:
            ref = tall.at[rz(z + off), c]
            send(ref, ref, ("p", max(abs(off), 1)), dev(x, y, z, 1 - c), "p")

    def t_passed(off):
        if ZC:
            got_texts((3, 2, 2, 1)[off - 1], ("p", off))

    both = (0, 1)

    def t_half(t, h):
        if ZC:
            with jax.named_scope(f"T{t}{h}"):
                got_texts(1, ("t", t, h))
            for d in both:
                if t < 3 or h == d:
                    t_send(d, t + 1, h)
            if h == 1:
                t_pass(-t)
                t_pass(t)

    def s_round(off):
        if XY:
            for d in both:
                got_images(2 if off == 1 else 1, ("s", off, d))
                for half in both:
                    for o in ((-1, 1) if off == 1 else (off,)):
                        second_send(half, o, d, 2)

    CW = NC * W

    def logits(shards, zs):
        lhs = jnp.concatenate([iall[i, j] for i, j in shards], axis=0)
        parts = [None, None]
        for zz in zs:
            cols = pl.ds(pl.multiple_of(zz * CW, W), CW)
            rhs = tall[zz].reshape(CW, D)
            dots = lax.dot_general(lhs, rhs, (((1,), (1,)), ((), ())), preferred_element_type=F32)
            lg = dots * scale2
            e = jnp.exp2(lg)
            el = e * lg
            for n, (i, j) in enumerate(shards):
                ee[i, j, :, cols] = e[n * W:(n + 1) * W]
            for m, (ref, val) in enumerate(((csum, e), (cel, el))):
                for k in range(NC):
                    part = val[:, k * W:(k + 1) * W]
                    parts[m] = part if parts[m] is None else parts[m] + part
                ref[:, cols] += jnp.sum(val.reshape(len(shards) * W // 8, 8, CW), axis=0)
        for ref, part in ((rsum, parts[0]), (rel, parts[1])):
            for n, (i, j) in enumerate(shards):
                ref[i, j] += part[n * W:(n + 1) * W]

    cross = [(x, y)]
    corners, across = [], []
    if XY:
        cross += [(rx(x - 1), y), (rx(x + 1), y), (x, ry(y - 1)), (x, ry(y + 1))]
        corners = [(rx(x + i), ry(y + j)) for i in (-1, 1) for j in (-1, 1)]
        across = [(x, ry(y + 2)), (rx(x + 2), y)]

    def tiles(name, shards, *offs):
        zs = [rz(z + off) for off in offs] if ZC else [z] if 0 in offs else []
        if shards and zs:
            with jax.named_scope(name):
                logits(shards, zs)

    def near(name, *offs):
        zs = [rz(z + off) for off in offs]

        def body(g, carry):
            i = rx(x + g - 1)
            logits([(i, ry(y - 1)), (i, y), (i, ry(y + 1))], zs)
            return carry

        with jax.named_scope(name):
            if ZC and XY:
                lax.fori_loop(0, 3, body, 0)
            elif ZC:
                logits(cross, zs)

    def whole(name, off):
        def body(i, carry):
            logits([(i, j) for j in range(NY)], [rz(z + off)])
            return carry

        with jax.named_scope(name):
            if ZC:
                lax.fori_loop(0, NX, body, 0)

    def far(name, pairs):
        with jax.named_scope(name):
            if not XY:
                return
            shards = [(rx(x - 1), ry(y + 2)), (rx(x + 1), ry(y + 2))] + [(rx(x + 2), ry(y + k)) for k in (-1, 1, 2)]

            def body(p, carry):
                logits(shards, [rz(z - p), rz(z + p)])
                return carry

            if not pairs:
                logits(shards, [z])
            elif ZC:
                lax.fori_loop(1, 4, body, 0)

    if XY:
        for half in both:
            for d in both:
                first_send(half, d, 1)
    if ZC:
        for h in both:
            for d in both:
                t_send(d, 1, h)
        t_pass(0)
    if XY:
        for half in both:
            for d in both:
                second_send(half, 0, d, 1)
        with jax.named_scope("f1"):
            for d in both:
                got_images(1, ("f", d))
                for half in both:
                    first_send(half, d, 2)
        for d in both:
            for half in both:
                for e in both:
                    second_send(half, -sg[d], e, 1)
    t_half(1, 0)
    t_half(1, 1)
    with jax.named_scope("s0"):
        s_round(0)
    if XY:
        with jax.named_scope("f2"):
            got_images(1, ("f2",))
        for half in both:
            for d in both:
                second_send(half, 2, d, 1)
    with jax.named_scope("p1"):
        t_passed(1)
    t_half(2, 0)
    tiles("C0", cross, -1, 0, 1)
    t_half(2, 1)
    with jax.named_scope("s1"):
        s_round(1)
    tiles("C1", corners, -1, 0, 1)
    t_half(3, 0)
    with jax.named_scope("p2"):
        t_passed(2)
    near("C2", -2, 2)
    with jax.named_scope("s0t2"):
        if XY:
            got_images(1, ("s2", True))
    tiles("C3", across, -2, -1, 0, 1, 2)
    t_half(3, 1)
    with jax.named_scope("s2"):
        s_round(2)
    with jax.named_scope("p3"):
        t_passed(3)
    near("C4", -3, 3)
    with jax.named_scope("T4"):
        if ZC:
            got_texts(1, ("t", 4, 0))
            t_pass(4)
    tiles("C4b", across, -3, 3)
    with jax.named_scope("end"):
        if XY:
            got_images(3, ("s2", False))
    far("C6", 1)
    far("C7", 0)
    with jax.named_scope("p4"):
        t_passed(4)
    whole("C5", 4)

    for k in range(NI):
        rall[mxy, k:k + 1, :] = jnp.sum(jnp.transpose(rsum[k // NY, k % NY]), axis=0, keepdims=True)
    for k in range(NT):
        call_[mzc, k:k + 1, :] = jnp.sum(csum[:, k * W:(k + 1) * W], axis=0, keepdims=True)

    def share(buf, key, peers, me, to, rows=None):
        ref = buf.at[me] if rows is None else buf.at[me, pl.ds(0, rows)]
        for p in peers:
            send(ref, ref, (key,), to(p), key)

    def shared(buf, key, peers, rows=None):
        if peers:
            ref = buf.at[pl.ds(0, len(peers))]
            got(ref if rows is None else ref.at[:, pl.ds(0, rows)], (key,))
        total = buf[0]
        for k in range(1, len(peers) + 1):
            total = total + buf[k]
        return total

    to_plane = lambda p: dev(p[1], p[2], z, c)
    to_line = lambda p: dev(x, y, p[1], p[2])
    share(rall, "r", plane, mxy, to_plane)
    share(call_, "c", line, mzc, to_line)
    with jax.named_scope("imgt"):
        for k in range(NI):
            tr = jnp.transpose(iall[k // NY, k % NY])
            for d in both:
                imgt[d, :, k * W:(k + 1) * W] = tr[d * H:(d + 1) * H]
        prod = iall[x, y].astype(F32) * tall[z, c].astype(F32)
        pos = prod[:, :W]
        for k in range(1, D // W):
            pos = pos + prod[:, k * W:(k + 1) * W]
        pos = scale * jnp.sum(pos, axis=0, keepdims=True)
    with jax.named_scope("rwait"):
        rtot = shared(rall, "r", plane)
    u = inv / rtot
    for k in range(NI):
        ub[k // NY, k % NY] = jnp.transpose(jnp.broadcast_to(u[k:k + 1, :], (W, W)))
    with jax.named_scope("cwait"):
        ctot = shared(call_, "c", line)
    v = inv / ctot
    uref[...] = rtot
    vref[...] = v

    def build(i, j):
        uu = ub[i, j]
        for k in range(NT):
            sl = slice(k * W, (k + 1) * W)
            gb[i, j, :, sl] = (ee[i, j, :, sl] * (uu + vref[k:k + 1, :])).astype(BF16)

    def builds(n, place):
        def body(k, carry):
            build(*place(k))
            return carry

        lax.fori_loop(0, n, body, 0)

    def unit_t(s):
        def body(d, carry):
            zz = rz(z - (1 - 2 * d) * (s + 1))
            rhs = gb[:, :, :, pl.ds(pl.multiple_of(zz * CW, W), CW)].reshape(NI * W, CW)
            res = jnp.dot(imgt[d], rhs, preferred_element_type=F32)
            for k in range(NC):
                ee[d * 2 + k, :, :, 1024 + s * W:1024 + (s + 1) * W] = res[:, k * W:(k + 1) * W].reshape(4, W, W)
            send(ee.at[d * 2 + 1 - c, :, :, pl.ds(1024 + s * W, W)], prt.at[d, s], ("w", s), dev(x, y, z, 1 - c), "w")
            return carry

        with jax.named_scope(f"ut{s}"):
            times[0] = 2
            lax.fori_loop(0, 2, body, 0)
            times[0] = 1

    def unit_i1(first, d, j):
        q = first * 2 + d
        step = (1 - 2 * d) * (j + 1)
        lhs = gb[:, ry(y - step)] if first == 0 else gb[rx(x - step)]
        rhs = tall[:, :, :, pl.ds(pl.multiple_of(q * Q, W), Q)].reshape(NT * W, Q)
        res = jnp.dot(lhs.reshape(4 * W, NT * W), rhs, preferred_element_type=F32)
        if j == 0:
            lead[q] = res.reshape(4, W, Q)
        else:
            ee[q, :, :, j * Q:(j + 1) * Q] = res.reshape(4, W, Q)

    def unit_i(first, j):
        def body(d, carry):
            unit_i1(first, d, j)
            return carry

        with jax.named_scope(f"ui{first}{j}"):
            lax.fori_loop(0, 2, body, 0)

    def i_dev(q, along_y, sign):
        return dev(x, ry(y + sign), z, c) if along_y else dev(rx(x + sign), y, z, c)

    def i_place(q, k):
        off = (2, sg[q % 2], -sg[q % 2], 0)[k]
        return rx(x + off) if q < 2 else ry(y + off)

    def i_step(d, j, k):
        got(recv1.at[0, 0, pl.ds(0, 2)], ("i", d, j - 1, k))
        for q in (d, d + 2):
            at, sign = i_place(q, k), sg[d]
            here = recv1.at[q, j - 1, at]
            here[...] += ee[q, at, :, j * Q:(j + 1) * Q]
            if j < 3:
                send(here, recv1.at[q, j, at], ("i", d, j, k), i_dev(q, q < 2, sign), "i")
            elif k == 0:
                send(here, recv2.at[q, 0], ("j", q, 0), i_dev(q, q >= 2, sign), "j")
            elif k == 2:
                send(here, recv2.at[q, 2], ("j", q, 2), i_dev(q, q >= 2, -sign), "j")

    def i_pass(q):
        here = recv2.at[q, 0]
        got(here, ("j", q, 0))
        here[...] += recv1[q, 2, i_place(q, 1)]
        send(here, recv2.at[q, 1], ("j", q, 1), i_dev(q, q >= 2, sg[q % 2]), "j")

    def i_last(q):
        got(recv2.at[q, 2], ("j", q, 2))
        got(recv2.at[q, 1], ("j", q, 1))
        block = recv1[q, 2, i_place(q, 3)] + recv2[q, 2] + recv2[q, 1]
        dimg_ref[:, q * Q:(q + 1) * Q] = (block * scale).astype(BF16)

    def z_step(s, k):
        if k == 0:
            got(prt.at[:, s], ("w", s))
        if s > 0:
            got(zrecv.at[:, s - 1, k], ("z", s - 1, k))
        for d in both:
            mine = ee.at[d * 2 + c, k, :, pl.ds(1024 + s * W, W)]
            if s == 0:
                mine[...] += prt[d, s, k]
                here = mine
            else:
                here = zrecv.at[d, s - 1, k]
            if s == 7:
                w = d * 4 + k
                block = here[...] + (mine[...] + prt[d, s, k])
                dtxt_ref[:, w * W:(w + 1) * W] = (jnp.transpose(block) * scale).astype(BF16)
                continue
            if s > 0:
                here[...] += mine[...] + prt[d, s, k]
            send(here, zrecv.at[d, s, k], ("z", s, k), dev(x, y, rz(z + sg[d]), c), "z")

    def totals():
        dts = jnp.zeros((8, W), F32)
        for k in range(NT):
            dts = dts + cel[:, k * W:(k + 1) * W] * vref[k:k + 1, :]

        def body(i, acc):
            for j in range(NY):
                acc = acc + jnp.sum((ub[i, j] * rel[i, j]).reshape(W // 8, 8, W), axis=0)
            return acc

        dts = lax.fori_loop(0, NX, body, dts)
        dt_part = jnp.sum(dts, axis=0, keepdims=True) * (1.0 / LOG2E) - (2.0 * inv) * pos
        loss = jnp.log(uref[pl.ds(mxy, 1), :]) - jnp.log(vref[pl.ds(mzc, 1), :] * (1.0 / inv)) - 2.0 * pos
        line_no = lax.broadcasted_iota(jnp.int32, (8, W), 0)
        sc1[mxy] = jnp.where(line_no == 0, jnp.broadcast_to(loss * inv, (8, W)),
                             jnp.where(line_no == 1, jnp.broadcast_to(dt_part, (8, W)), 0.0))
        share(sc1, "m", plane, mxy, to_plane, 2)

    def totals2():
        sc2[mzc] = shared(sc1, "m", plane, 2)
        share(sc2, "n", line, mzc, to_line, 2)

    def start(d):
        sign = sg[d]
        builds(4 - d, lambda k: (rx(x + k), ry(y - sign)))
        builds(3 - d, lambda k: (rx(x - sign), ry(y + k * (1 + d))))

    def start_send(d):
        for first in both:
            unit_i1(first, d, 0)
        for k in range(4):
            for q in (d, d + 2):
                place = i_place(q, k)
                send(lead.at[q, place], recv1.at[q, 0, place], ("i", d, 0, k), i_dev(q, q < 2, sg[d]), "i")

    if XY:
        with jax.named_scope("start0"):
            start(0)
            start_send(0)
        with jax.named_scope("start1"):
            start(1)
            start_send(1)
            builds(4, lambda k: (rx(x + 2 * lax.div(k, 2)), ry(y + 2 * lax.rem(k, 2))))
    else:
        build(0, 0)
    own = pl.ds(pl.multiple_of(mzc * W, W), W)
    eye = lax.broadcasted_iota(jnp.int32, (W, W), 0) == lax.broadcasted_iota(jnp.int32, (W, W), 1)
    gb[x, y, :, own] = (ee[x, y, :, own] * (ub[x, y] + vref[pl.ds(mzc, 1), :])
                        - jnp.where(eye, 2.0 * inv, 0.0)).astype(BF16)
    STEP, SUB, Z0 = 5.65, 2.82, 5.6
    base = (0.0, 2.0)
    events = []

    def at(time, fn, *args):
        events.append((time, len(events), fn, args))

    def z_time(s, k):
        return Z0 + (s - 1) * STEP + 1.7 + SUB / 2 * (k + 1) if s else Z0

    if ZC:
        for s, slot in ((0, 0.0), (1, 4.5), (2, Z0 + 0.05), (3, z_time(1, 3)), (4, z_time(2, 3)), (5, z_time(4, 1)),
                        (6, z_time(4, 3)), (7, z_time(5, 1))):
            at(slot + 0.01, unit_t, s)
        for s in range(8):
            for k in range(4):
                at(z_time(s, k), z_step, s, k)
    if XY:
        for first, slots in ((0, (Z0, z_time(1, 1), z_time(3, 1))), (1, (Z0, z_time(2, 1), z_time(3, 3)))):
            for j in range(1, 4):
                at(slots[j - 1] + 0.02, unit_i, first, j)
        for d in both:
            for j in range(1, 4):
                for k in range(4):
                    wait = (base[d] + 1.7 + (j - 1) * 2 * STEP + (k + 1) * SUB + (1.8, 2.0, 0.8)[j - 1])
                    at(max(wait, Z0 + 0.03) if j == 1 else wait, i_step, d, j, k)
            for q in (d, d + 2):
                at(base[d] + 38.5, i_pass, q)
                at(base[d] + 44.0, i_last, q)
    at(z_time(1, 1) + 0.015, totals)
    at(25.0, totals2)
    order = [(fn.__name__,) + args for _, _, fn, args in sorted(events, key=lambda e: e[:2])]
    for n, e in enumerate(order):
        if e[0] == "i_step":
            assert all(("unit_i", f, e[2]) in order[:n] for f in both)
        if e[0] == "z_step":
            assert ("unit_t", e[1]) in order[:n]
    for _, _, fn, args in sorted(events, key=lambda e: e[:2]):
        with jax.named_scope("_".join([fn.__name__] + [str(v) for v in args])):
            fn(*args)

    if not XY:
        for q in range(4):
            rhs = tall[:, :, :, q * Q:(q + 1) * Q].reshape(NT * W, Q)
            res = jnp.dot(gb[0, 0], rhs, preferred_element_type=F32)
            dimg_ref[:, q * Q:(q + 1) * Q] = (res * scale).astype(BF16)
    if not ZC:
        for d in both:
            res = jnp.dot(imgt[d], gb[...].reshape(NI * W, W), preferred_element_type=F32)
            for k in range(4):
                w = d * 4 + k
                dtxt_ref[:, w * W:(w + 1) * W] = (jnp.transpose(res[k * W:(k + 1) * W]) * scale).astype(BF16)
    with jax.named_scope("fin"):
        total = shared(sc2, "n", line, 2)
        scal_ref[...] = jnp.broadcast_to(jnp.sum(total, axis=1, keepdims=True), (8, W))
    for group, size in sent.items():
        if group in ("m", "n"):
            ref = (sc1 if group == "m" else sc2).at[pl.ds(0, size // 1024), pl.ds(0, 2)]
            pltpu.make_async_remote_copy(
                src_ref=ref, dst_ref=ref, send_sem=ssem.at[sid(group)], recv_sem=rsem.at[0],
                device_id=dev(x, y, z, c), device_id_type=MESH).wait_send()
            continue
        a, b, r, l = block_of(size // 4096)
        ref = ee.at[pl.ds(0, a), pl.ds(0, b), pl.ds(0, r), pl.ds(0, l)]
        pltpu.make_async_remote_copy(
            src_ref=ref, dst_ref=ref, send_sem=ssem.at[sid(group)], recv_sem=rsem.at[0],
            device_id=dev(x, y, z, c), device_id_type=MESH).wait_send()
    assert len(sid.ids) <= N_SEND and len(rid.ids) <= N_RECV, (len(sid.ids), len(rid.ids))

def call(NX, NY, NZ, NC, scale, img, txt):
    D = img.shape[1]
    NI, NT = NX * NY, NZ * NC
    H, Q = D // 2, D // 4
    vmem = pltpu.VMEM
    return pl.pallas_call(
        functools.partial(kernel, NX, NY, NZ, NC),
        out_shape=(jax.ShapeDtypeStruct(img.shape, BF16), jax.ShapeDtypeStruct(txt.shape, BF16),
                   jax.ShapeDtypeStruct((8, W), F32)),
        in_specs=[pl.BlockSpec(memory_space=pltpu.SMEM)] + [pl.BlockSpec(memory_space=pl.ANY)] * 2,
        out_specs=[pl.BlockSpec(memory_space=vmem)] * 3,
        scratch_shapes=[
            vmem((NX, NY, W, D), BF16), vmem((NZ, NC, W, D), BF16), vmem((2, H, NI * W), BF16),
            vmem((4, 4, W, 2048), F32), vmem((NX, NY, W, NT * W), BF16),
            vmem((NX, NY, W, W), F32), vmem((NX, NY, W, W), F32), vmem((8, NT * W), F32), vmem((8, NT * W), F32),
            vmem((NI, NI, W), F32), vmem((NT, NT, W), F32), vmem((NI, W), F32), vmem((NT, W), F32),
            vmem((NX, NY, W, W), F32), vmem((NI, 8, W), F32), vmem((NT, 8, W), F32),
            vmem((4, 3, 4, W, Q), F32), vmem((4, 3, W, Q), F32),
            vmem((2, 8, 4, W, W), F32), vmem((2, 7, 4, W, W), F32), vmem((4, 4, W, Q), F32),
            pltpu.SemaphoreType.DMA((N_SEND,)), pltpu.SemaphoreType.DMA((N_RECV,)),
            pltpu.SemaphoreType.DMA((2,)),
        ],
        compiler_params=pltpu.CompilerParams(collective_id=0, has_side_effects=True, vmem_limit_bytes=67043328),
    )(scale, img, txt)


def finish(img_ref, txt_ref, scal_ref, dimg_ref, dtxt_ref, loss_ref, dt_ref):
    dimg_ref[...] = img_ref[...]
    dtxt_ref[...] = txt_ref[...]
    loss_ref[0, 0] = scal_ref[0, 0]
    dt_ref[0, 0] = scal_ref[1, 0]


SHAPE = (4, 4, 8, 2)


def solution(mesh):
    batch_spec = P(("row", "col"), None)

    def local_tile(img_loc, txt_loc, log_scale):
        scale = jnp.exp(log_scale).reshape(1, 1)
        d_img, d_txt, scal = call(*SHAPE, scale, img_loc, txt_loc)
        vmem = pl.BlockSpec(memory_space=pltpu.VMEM)
        smem = pl.BlockSpec(memory_space=pltpu.SMEM)
        one = jax.ShapeDtypeStruct((1, 1), F32)
        d_img, d_txt, loss, d_scale = pl.pallas_call(
            finish, out_shape=(jax.ShapeDtypeStruct(d_img.shape, BF16), jax.ShapeDtypeStruct(d_txt.shape, BF16), one, one),
            in_specs=[vmem, vmem, smem], out_specs=[vmem, vmem, smem, smem])(d_img, d_txt, scal)
        return loss[0, 0], d_img, d_txt, d_scale[0, 0]

    return jax.shard_map(local_tile, mesh=mesh, in_specs=(batch_spec, batch_spec, P()),
                         out_specs=(P(), batch_spec, batch_spec, P()), check_vma=False)
```

```python
import functools

import jax
import jax.numpy as jnp
from jax import lax
from jax.experimental import pallas as pl
from jax.experimental.pallas import tpu as pltpu
from jax.sharding import PartitionSpec as P

MESH = pl.DeviceIdType.MESH
F32 = jnp.float32
LOG2E = 1.4426950408889634
BF16 = jnp.bfloat16
W = 128


N_SEND, N_RECV = 14, 98


class Names:
    def __init__(self):
        self.ids = {}

    def __call__(self, *key):
        return self.ids.setdefault(key, len(self.ids))


def block_of(tiles):
    for a in range(1, 5):
        for b in range(1, 5):
            for r in range(1, 17):
                if tiles % (a * b * r) == 0 and tiles // (a * b * r) <= 16:
                    return a, b, r * 8, tiles // (a * b * r) * 128
    raise ValueError(tiles)


def kernel(NX, NY, NZ, NC, scale_ref, img_ref, txt_ref, dimg_ref, dtxt_ref, scal_ref,
           iall, tall, imgt, ee, gb, rsum, rel, csum, cel, rall, call_, uref, vref, ub, sc1, sc2,
           recv1, recv2, prt, zrecv, lead, ssem, rsem, lsem):
    D = img_ref.shape[1]
    NI, NT = NX * NY, NZ * NC
    XY, ZC = NI > 1, NT > 1
    H, Q = D // 2, D // 4
    inv = 1.0 / (2.0 * W * NI * NT)
    row, col = lax.axis_index("row"), lax.axis_index("col")
    x, c = lax.div(row, NC), lax.rem(row, NC)
    z, y = lax.div(col, NY), lax.rem(col, NY)
    mxy, mzc = x * NY + y, z * NC + c
    scale = scale_ref[0, 0]
    scale2 = scale * LOG2E
    rx = lambda v: lax.rem(v + 2 * NX, NX)
    ry = lambda v: lax.rem(v + 2 * NY, NY)
    rz = lambda v: lax.rem(v + 2 * NZ, NZ)

    def dev(px, py, pz, pc):
        return (pz * NY + py, px * NC + pc)

    plane = [(p, rx(x + p // NY), ry(y + p % NY)) for p in range(1, NI)]
    line = [(p, rz(z + p // NC), lax.rem(c + p % NC, NC)) for p in range(1, NT)]
    near_x, near_z = (lambda k: min(k, NX - k)), (lambda k: min(k, NZ - k))
    plane.sort(key=lambda p: -near_x(p[0] // NY) - near_x(p[0] % NY))
    line.sort(key=lambda p: -near_z(p[0] // NC) * NC - p[0] % NC)
    barrier = pltpu.get_barrier_semaphore()
    greet = []
    if XY:
        greet += [dev(rx(x + k), y, z, c) for k in (1, -1)] + [dev(x, ry(y + k), z, c) for k in (1, -1)]
    if ZC:
        greet += [dev(x, y, rz(z + k), c) for k in (1, -1)] + [dev(x, y, z, 1 - c)]
    for device in greet:
        pl.semaphore_signal(barrier, inc=1, device_id=device, device_id_type=MESH)
    loads = [pltpu.make_async_copy(img_ref, iall.at[x, y], lsem.at[0]), pltpu.make_async_copy(txt_ref, tall.at[z, c], lsem.at[1])]
    for load in loads:
        load.start()
    for ref in (csum, cel, rsum, rel, sc1, sc2):
        ref[...] = jnp.zeros_like(ref)
    with jax.named_scope("barrier"):
        for load in loads:
            load.wait()
        pl.semaphore_wait(barrier, len(greet))

    rid, sid = Names(), Names()
    sent = {}
    times = [1]

    def send(src, dst, key, device, group, offset=0):
        pltpu.make_async_remote_copy(
            src_ref=src, dst_ref=dst, send_sem=ssem.at[sid(group)], recv_sem=rsem.at[rid(*key) + offset],
            device_id=device, device_id_type=MESH).start()
        size = jnp.dtype(src.dtype).itemsize
        for n in src.shape:
            size *= n
        sent[group] = sent.get(group, 0) + size * times[0]

    def got(dst, key):
        pltpu.make_async_remote_copy(
            src_ref=dst, dst_ref=dst, send_sem=ssem.at[0], recv_sem=rsem.at[rid(*key)],
            device_id=dev(x, y, z, c), device_id_type=MESH).wait_recv()

    sg = (1, -1)
    lo, full = W // 4, W // 2

    def rows(half, part=None):
        start, size = half * full, full
        if part is not None:
            start, size = start + part * lo, lo
        return pl.ds(start, size)

    def first_dev(half, d):
        return dev(rx(x + sg[d]), y, z, c) if half == 0 else dev(x, ry(y + sg[d]), z, c)

    def second_dev(half, d):
        return dev(x, ry(y + sg[d]), z, c) if half == 0 else dev(rx(x + sg[d]), y, z, c)

    def first_piece(half, off):
        return (rx(x + off), y) if half == 0 else (x, ry(y + off))

    def second_piece(half, off1, off2):
        return (rx(x + off1), ry(y + off2)) if half == 0 else (rx(x + off2), ry(y + off1))

    def ipc(pc, sl):
        return iall.at[pc[0], pc[1], sl]

    def got_images(shards, key):
        got(iall.at[0, pl.ds(0, shards)], key)

    def got_texts(shards, key):
        got(tall.at[pl.ds(0, shards), 0], key)

    def first_send(half, d, t):
        if t == 1:
            ref = ipc((x, y), rows(half))
            send(ref, ref, ("f", d), first_dev(half, d), "f1")
        else:
            ref = ipc(first_piece(half, -sg[d]), rows(half, d))
            send(ref, ref, ("f2",), first_dev(half, d), "f2")

    def second_send(half, off, d, t):
        if t == 1:
            ref = ipc(second_piece(half, off, 0), rows(half))
            send(ref, ref, ("s", abs(off), d), second_dev(half, d), "s1")
        else:
            ref = ipc(second_piece(half, off, -sg[d]), rows(half, d))
            send(ref, ref, ("s2", off == 0), second_dev(half, d), "s2")

    def t_send(d, t, h):
        ref = tall.at[rz(z - sg[d] * (t - 1)), c, rows(h)]
        send(ref, ref, ("t", t, h if t < 4 else 0), dev(x, y, rz(z + sg[d]), c), "t")

    def t_pass(off, *part):
        if ZC:
            ref = tall.at[rz(z + off), c]
            ref = ref.at[rows(*part)] if part else ref
            send(ref, ref, ("p", max(abs(off), 1)), dev(x, y, z, 1 - c), "p")

    def t_passed(off):
        if ZC:
            got_texts((3, 2, 2, 1)[off - 1], ("p", off))

    both = (0, 1)

    def t_half(t, h):
        if ZC:
            with jax.named_scope(f"T{t}{h}"):
                got_texts(1, ("t", t, h))
            for d in both:
                if t < 3 or h == d:
                    t_send(d, t + 1, h)
            t_pass(-t, h)
            t_pass(t, h)

    def s_round(off):
        if XY:
            for d in both:
                got_images(2 if off == 1 else 1, ("s", off, d))
                for half in both:
                    for o in ((-1, 1) if off == 1 else (off,)):
                        second_send(half, o, d, 2)

    CW = NC * W

    def logits(shards, zs):
        lhs = jnp.concatenate([iall[i, j] for i, j in shards], axis=0)
        parts = [None, None]
        for zz in zs:
            cols = pl.ds(pl.multiple_of(zz * CW, W), CW)
            rhs = tall[zz].reshape(CW, D)
            dots = lax.dot_general(lhs, rhs, (((1,), (1,)), ((), ())), preferred_element_type=F32)
            lg = dots * scale2
            e = jnp.exp2(lg)
            el = e * lg
            for n, (i, j) in enumerate(shards):
                ee[i, j, :, cols] = e[n * W:(n + 1) * W]
            for m, (ref, val) in enumerate(((csum, e), (cel, el))):
                for k in range(NC):
                    part = val[:, k * W:(k + 1) * W]
                    parts[m] = part if parts[m] is None else parts[m] + part
                ref[:, cols] += jnp.sum(val.reshape(len(shards) * W // 8, 8, CW), axis=0)
        for ref, part in ((rsum, parts[0]), (rel, parts[1])):
            for n, (i, j) in enumerate(shards):
                ref[i, j] += part[n * W:(n + 1) * W]

    cross = [(x, y)]
    corners, across = [], []
    if XY:
        cross += [(rx(x - 1), y), (rx(x + 1), y), (x, ry(y - 1)), (x, ry(y + 1))]
        corners = [(rx(x + i), ry(y + j)) for i in (-1, 1) for j in (-1, 1)]
        across = [(x, ry(y + 2)), (rx(x + 2), y)]

    def tiles(name, shards, *offs):
        zs = [rz(z + off) for off in offs] if ZC else [z] if 0 in offs else []
        if shards and zs:
            with jax.named_scope(name):
                logits(shards, zs)

    def near(name, *offs):
        zs = [rz(z + off) for off in offs]

        def body(g, carry):
            i = rx(x + g - 1)
            logits([(i, ry(y - 1)), (i, y), (i, ry(y + 1))], zs)
            return carry

        with jax.named_scope(name):
            if ZC and XY:
                lax.fori_loop(0, 3, body, 0)
            elif ZC:
                logits(cross, zs)

    def whole(name, off):
        def body(i, carry):
            logits([(i, j) for j in range(NY)], [rz(z + off)])
            return carry

        with jax.named_scope(name):
            if ZC:
                lax.fori_loop(0, NX, body, 0)

    def far(name, pairs):
        with jax.named_scope(name):
            if not XY:
                return
            shards = [(rx(x - 1), ry(y + 2)), (rx(x + 1), ry(y + 2))] + [(rx(x + 2), ry(y + k)) for k in (-1, 1, 2)]

            def body(p, carry):
                logits(shards, [rz(z - p), rz(z + p)])
                return carry

            if not pairs:
                logits(shards, [z])
            elif ZC:
                lax.fori_loop(1, 4, body, 0)

    if XY:
        for half in both:
            for d in both:
                first_send(half, d, 1)
    if ZC:
        for h in both:
            for d in both:
                t_send(d, 1, h)
        t_pass(0)
    if XY:
        for half in both:
            for d in both:
                second_send(half, 0, d, 1)
        with jax.named_scope("f1"):
            for d in both:
                got_images(1, ("f", d))
                for half in both:
                    first_send(half, d, 2)
        for d in both:
            for half in both:
                for e in both:
                    second_send(half, -sg[d], e, 1)
    t_half(1, 0)
    t_half(1, 1)
    with jax.named_scope("s0"):
        s_round(0)
    if XY:
        with jax.named_scope("f2"):
            got_images(1, ("f2",))
        for half in both:
            for d in both:
                second_send(half, 2, d, 1)
    with jax.named_scope("p1"):
        t_passed(1)
    t_half(2, 0)
    tiles("C0", cross, -1, 0, 1)
    t_half(2, 1)
    with jax.named_scope("s1"):
        s_round(1)
    tiles("C1", corners, -1, 0, 1)
    t_half(3, 0)
    with jax.named_scope("p2"):
        t_passed(2)
    near("C2", -2, 2)
    with jax.named_scope("s0t2"):
        if XY:
            got_images(1, ("s2", True))
    tiles("C3", across, -2, -1, 0, 1, 2)
    t_half(3, 1)
    with jax.named_scope("s2"):
        s_round(2)
    with jax.named_scope("p3"):
        t_passed(3)
    near("C4", -3, 3)
    with jax.named_scope("T4"):
        if ZC:
            got_texts(1, ("t", 4, 0))
            t_pass(4)
    tiles("C4b", across, -3, 3)
    with jax.named_scope("end"):
        if XY:
            got_images(3, ("s2", False))
    far("C6", 1)
    far("C7", 0)
    with jax.named_scope("p4"):
        t_passed(4)
    whole("C5", 4)

    def share(buf, key, peers, me, to, rows=None):
        ref = buf.at[me] if rows is None else buf.at[me, pl.ds(0, rows)]
        for p in peers:
            send(ref, ref, (key,), to(p), key)

    def shared(buf, key, peers, rows=None):
        if peers:
            ref = buf.at[pl.ds(0, len(peers))]
            got(ref if rows is None else ref.at[:, pl.ds(0, rows)], (key,))
        total = buf[0]
        for k in range(1, len(peers) + 1):
            total = total + buf[k]
        return total

    to_plane = lambda p: dev(p[1], p[2], z, c)
    to_line = lambda p: dev(x, y, p[1], p[2])
    for k in range(NT):
        call_[mzc, k:k + 1, :] = jnp.sum(csum[:, k * W:(k + 1) * W], axis=0, keepdims=True)
    share(call_, "c", line, mzc, to_line)
    for k in range(NI):
        rall[mxy, k:k + 1, :] = jnp.sum(jnp.transpose(rsum[k // NY, k % NY]), axis=0, keepdims=True)
    share(rall, "r", plane, mxy, to_plane)
    with jax.named_scope("imgt"):
        for k in range(NI):
            tr = jnp.transpose(iall[k // NY, k % NY])
            for d in both:
                imgt[d, :, k * W:(k + 1) * W] = tr[d * H:(d + 1) * H]
        prod = iall[x, y].astype(F32) * tall[z, c].astype(F32)
        pos = prod[:, :W]
        for k in range(1, D // W):
            pos = pos + prod[:, k * W:(k + 1) * W]
        pos = scale * jnp.sum(pos, axis=0, keepdims=True)
    with jax.named_scope("rwait"):
        rtot = shared(rall, "r", plane)
    u = inv / rtot
    for k in range(NI):
        ub[k // NY, k % NY] = jnp.transpose(jnp.broadcast_to(u[k:k + 1, :], (W, W)))
    with jax.named_scope("cwait"):
        ctot = shared(call_, "c", line)
    v = inv / ctot
    uref[...] = rtot
    vref[...] = v

    def build(i, j):
        uu = ub[i, j]
        for k in range(NT):
            sl = slice(k * W, (k + 1) * W)
            gb[i, j, :, sl] = (ee[i, j, :, sl] * (uu + vref[k:k + 1, :])).astype(BF16)

    def builds(n, place):
        def body(k, carry):
            build(*place(k))
            return carry

        lax.fori_loop(0, n, body, 0)

    def unit_t(s):
        def body(d, carry):
            zz = rz(z - (1 - 2 * d) * (s + 1))
            rhs = gb[:, :, :, pl.ds(pl.multiple_of(zz * CW, W), CW)].reshape(NI * W, CW)
            res = jnp.dot(imgt[d], rhs, preferred_element_type=F32)
            for k in range(NC):
                ee[d * 2 + k, :, :, 1024 + s * W:1024 + (s + 1) * W] = res[:, k * W:(k + 1) * W].reshape(4, W, W)
            send(ee.at[d * 2 + 1 - c, :, :, pl.ds(1024 + s * W, W)], prt.at[d, s], ("w", s), dev(x, y, z, 1 - c), "w")
            return carry

        with jax.named_scope(f"ut{s}"):
            times[0] = 2
            lax.fori_loop(0, 2, body, 0)
            times[0] = 1

    def unit_i1(first, d, j):
        q = first * 2 + d
        step = (1 - 2 * d) * (j + 1)
        lhs = gb[:, ry(y - step)] if first == 0 else gb[rx(x - step)]
        rhs = tall[:, :, :, pl.ds(pl.multiple_of(q * Q, W), Q)].reshape(NT * W, Q)
        res = jnp.dot(lhs.reshape(4 * W, NT * W), rhs, preferred_element_type=F32)
        if j == 0:
            lead[q] = res.reshape(4, W, Q)
        else:
            ee[q, :, :, j * Q:(j + 1) * Q] = res.reshape(4, W, Q)

    def unit_i(first, j):
        def body(d, carry):
            unit_i1(first, d, j)
            return carry

        with jax.named_scope(f"ui{first}{j}"):
            lax.fori_loop(0, 2, body, 0)

    def i_dev(q, along_y, sign):
        return dev(x, ry(y + sign), z, c) if along_y else dev(rx(x + sign), y, z, c)

    def i_place(q, k):
        off = (2, sg[q % 2], -sg[q % 2], 0)[k]
        return rx(x + off) if q < 2 else ry(y + off)

    def i_step(d, j, k):
        got(recv1.at[0, 0, pl.ds(0, 2)], ("i", d, j - 1, k))
        for q in (d, d + 2):
            at, sign = i_place(q, k), sg[d]
            here = recv1.at[q, j - 1, at]
            here[...] += ee[q, at, :, j * Q:(j + 1) * Q]
            if j < 3:
                send(here, recv1.at[q, j, at], ("i", d, j, k), i_dev(q, q < 2, sign), "i")
            elif k == 0:
                send(here, recv2.at[q, 0], ("j", q, 0), i_dev(q, q >= 2, sign), "j")
            elif k == 2:
                send(here, recv2.at[q, 2], ("j", q, 2), i_dev(q, q >= 2, -sign), "j")

    def i_pass(q):
        here = recv2.at[q, 0]
        got(here, ("j", q, 0))
        here[...] += recv1[q, 2, i_place(q, 1)]
        send(here, recv2.at[q, 1], ("j", q, 1), i_dev(q, q >= 2, sg[q % 2]), "j")

    def i_last(q):
        got(recv2.at[q, 2], ("j", q, 2))
        got(recv2.at[q, 1], ("j", q, 1))
        block = recv1[q, 2, i_place(q, 3)] + recv2[q, 2] + recv2[q, 1]
        dimg_ref[:, q * Q:(q + 1) * Q] = (block * scale).astype(BF16)

    def z_step(s, k):
        if k == 0:
            got(prt.at[:, s], ("w", s))
        if s > 0:
            got(zrecv.at[:, s - 1, k], ("z", s - 1, k))
        for d in both:
            mine = ee.at[d * 2 + c, k, :, pl.ds(1024 + s * W, W)]
            if s == 0:
                mine[...] += prt[d, s, k]
                here = mine
            else:
                here = zrecv.at[d, s - 1, k]
            if s == 7:
                w = d * 4 + k
                block = here[...] + (mine[...] + prt[d, s, k])
                dtxt_ref[:, w * W:(w + 1) * W] = (jnp.transpose(block) * scale).astype(BF16)
                continue
            if s > 0:
                here[...] += mine[...] + prt[d, s, k]
            send(here, zrecv.at[d, s, k], ("z", s, k), dev(x, y, rz(z + sg[d]), c), "z")

    def totals():
        dts = jnp.zeros((8, W), F32)
        for k in range(NT):
            dts = dts + cel[:, k * W:(k + 1) * W] * vref[k:k + 1, :]

        def body(i, acc):
            for j in range(NY):
                acc = acc + jnp.sum((ub[i, j] * rel[i, j]).reshape(W // 8, 8, W), axis=0)
            return acc

        dts = lax.fori_loop(0, NX, body, dts)
        dt_part = jnp.sum(dts, axis=0, keepdims=True) * (1.0 / LOG2E) - (2.0 * inv) * pos
        loss = jnp.log(uref[pl.ds(mxy, 1), :]) - jnp.log(vref[pl.ds(mzc, 1), :] * (1.0 / inv)) - 2.0 * pos
        line_no = lax.broadcasted_iota(jnp.int32, (8, W), 0)
        sc1[mxy] = jnp.where(line_no == 0, jnp.broadcast_to(loss * inv, (8, W)),
                             jnp.where(line_no == 1, jnp.broadcast_to(dt_part, (8, W)), 0.0))
        share(sc1, "m", plane, mxy, to_plane, 2)

    def totals2():
        sc2[mzc] = shared(sc1, "m", plane, 2)
        share(sc2, "n", line, mzc, to_line, 2)

    def start(d):
        sign = sg[d]
        builds(4 - d, lambda k: (rx(x + k), ry(y - sign)))
        builds(3 - d, lambda k: (rx(x - sign), ry(y + k * (1 + d))))

    def start_send(d):
        for first in both:
            unit_i1(first, d, 0)
        for k in range(4):
            for q in (d, d + 2):
                place = i_place(q, k)
                send(lead.at[q, place], recv1.at[q, 0, place], ("i", d, 0, k), i_dev(q, q < 2, sg[d]), "i")

    if XY:
        with jax.named_scope("start0"):
            start(0)
            start_send(0)
        with jax.named_scope("start1"):
            start(1)
            start_send(1)
            builds(4, lambda k: (rx(x + 2 * lax.div(k, 2)), ry(y + 2 * lax.rem(k, 2))))
    else:
        build(0, 0)
    own = pl.ds(pl.multiple_of(mzc * W, W), W)
    eye = lax.broadcasted_iota(jnp.int32, (W, W), 0) == lax.broadcasted_iota(jnp.int32, (W, W), 1)
    gb[x, y, :, own] = (ee[x, y, :, own] * (ub[x, y] + vref[pl.ds(mzc, 1), :])
                        - jnp.where(eye, 2.0 * inv, 0.0)).astype(BF16)
    STEP, SUB, Z0 = 5.65, 2.82, 5.6
    base = (0.0, 2.0)
    events = []

    def at(time, fn, *args):
        events.append((time, len(events), fn, args))

    def z_time(s, k):
        return Z0 + (s - 1) * STEP + 1.7 + SUB / 2 * (k + 1) if s else Z0

    if ZC:
        for s, slot in ((0, 0.0), (1, 4.5), (2, Z0 + 0.05), (3, z_time(1, 3)), (4, z_time(2, 3)), (5, z_time(4, 1)),
                        (6, z_time(4, 3)), (7, z_time(5, 1))):
            at(slot + 0.01, unit_t, s)
        for s in range(8):
            for k in range(4):
                at(z_time(s, k), z_step, s, k)
    if XY:
        for first, slots in ((0, (Z0, z_time(1, 1), z_time(3, 1))), (1, (Z0, z_time(2, 1), z_time(3, 3)))):
            for j in range(1, 4):
                at(slots[j - 1] + 0.02, unit_i, first, j)
        for d in both:
            for j in range(1, 4):
                for k in range(4):
                    wait = (base[d] + 1.7 + (j - 1) * 2 * STEP + (k + 1) * SUB + (1.8, 2.0, 0.8)[j - 1])
                    at(max(wait, Z0 + 0.03) if j == 1 else wait, i_step, d, j, k)
            for q in (d, d + 2):
                at(base[d] + 38.5, i_pass, q)
                at(base[d] + 44.0, i_last, q)
    at(z_time(1, 1) + 0.015, totals)
    at(25.0, totals2)
    for _, _, fn, args in sorted(events, key=lambda e: e[:2]):
        with jax.named_scope("_".join([fn.__name__] + [str(v) for v in args])):
            fn(*args)

    with jax.named_scope("fin"):
        total = shared(sc2, "n", line, 2)
        scal_ref[...] = jnp.broadcast_to(jnp.sum(total, axis=1, keepdims=True), (8, W))
    for group, size in sent.items():
        if group in ("m", "n"):
            ref = (sc1 if group == "m" else sc2).at[pl.ds(0, size // 1024), pl.ds(0, 2)]
            pltpu.make_async_remote_copy(
                src_ref=ref, dst_ref=ref, send_sem=ssem.at[sid(group)], recv_sem=rsem.at[0],
                device_id=dev(x, y, z, c), device_id_type=MESH).wait_send()
            continue
        a, b, r, l = block_of(size // 4096)
        ref = ee.at[pl.ds(0, a), pl.ds(0, b), pl.ds(0, r), pl.ds(0, l)]
        pltpu.make_async_remote_copy(
            src_ref=ref, dst_ref=ref, send_sem=ssem.at[sid(group)], recv_sem=rsem.at[0],
            device_id=dev(x, y, z, c), device_id_type=MESH).wait_send()
    assert len(sid.ids) <= N_SEND and len(rid.ids) <= N_RECV, (len(sid.ids), len(rid.ids))

def call(NX, NY, NZ, NC, scale, img, txt):
    D = img.shape[1]
    NI, NT = NX * NY, NZ * NC
    H, Q = D // 2, D // 4
    vmem = pltpu.VMEM
    return pl.pallas_call(
        functools.partial(kernel, NX, NY, NZ, NC),
        out_shape=(jax.ShapeDtypeStruct(img.shape, BF16), jax.ShapeDtypeStruct(txt.shape, BF16),
                   jax.ShapeDtypeStruct((8, W), F32)),
        in_specs=[pl.BlockSpec(memory_space=pltpu.SMEM)] + [pl.BlockSpec(memory_space=pl.ANY)] * 2,
        out_specs=[pl.BlockSpec(memory_space=vmem)] * 3,
        scratch_shapes=[
            vmem((NX, NY, W, D), BF16), vmem((NZ, NC, W, D), BF16), vmem((2, H, NI * W), BF16),
            vmem((4, 4, W, 2048), F32), vmem((NX, NY, W, NT * W), BF16),
            vmem((NX, NY, W, W), F32), vmem((NX, NY, W, W), F32), vmem((8, NT * W), F32), vmem((8, NT * W), F32),
            vmem((NI, NI, W), F32), vmem((NT, NT, W), F32), vmem((NI, W), F32), vmem((NT, W), F32),
            vmem((NX, NY, W, W), F32), vmem((NI, 8, W), F32), vmem((NT, 8, W), F32),
            vmem((4, 3, 4, W, Q), F32), vmem((4, 3, W, Q), F32),
            vmem((2, 8, 4, W, W), F32), vmem((2, 7, 4, W, W), F32), vmem((4, 4, W, Q), F32),
            pltpu.SemaphoreType.DMA((N_SEND,)), pltpu.SemaphoreType.DMA((N_RECV,)),
            pltpu.SemaphoreType.DMA((2,)),
        ],
        compiler_params=pltpu.CompilerParams(collective_id=0, has_side_effects=True, vmem_limit_bytes=67043328),
    )(scale, img, txt)


def finish(img_ref, txt_ref, scal_ref, dimg_ref, dtxt_ref, loss_ref, dt_ref):
    dimg_ref[...] = img_ref[...]
    dtxt_ref[...] = txt_ref[...]
    loss_ref[0, 0] = scal_ref[0, 0]
    dt_ref[0, 0] = scal_ref[1, 0]


SHAPE = (4, 4, 8, 2)


def solution(mesh):
    batch_spec = P(("row", "col"), None)

    def local_tile(img_loc, txt_loc, log_scale):
        scale = jnp.exp(log_scale).reshape(1, 1)
        d_img, d_txt, scal = call(*SHAPE, scale, img_loc, txt_loc)
        vmem = pl.BlockSpec(memory_space=pltpu.VMEM)
        smem = pl.BlockSpec(memory_space=pltpu.SMEM)
        one = jax.ShapeDtypeStruct((1, 1), F32)
        d_img, d_txt, loss, d_scale = pl.pallas_call(
            finish, out_shape=(jax.ShapeDtypeStruct(d_img.shape, BF16), jax.ShapeDtypeStruct(d_txt.shape, BF16), one, one),
            in_specs=[vmem, vmem, smem], out_specs=[vmem, vmem, smem, smem])(d_img, d_txt, scal)
        return loss[0, 0], d_img, d_txt, d_scale[0, 0]

    return jax.shard_map(local_tile, mesh=mesh, in_specs=(batch_spec, batch_spec, P()),
                         out_specs=(P(), batch_spec, batch_spec, P()), check_vma=False)
```

```python
import functools

import jax
import jax.numpy as jnp
from jax import lax
from jax.experimental import pallas as pl
from jax.experimental.pallas import tpu as pltpu
from jax.sharding import PartitionSpec as P

MESH = pl.DeviceIdType.MESH
F32 = jnp.float32
LOG2E = 1.4426950408889634
BF16 = jnp.bfloat16
W = 128


N_SEND, N_RECV = 14, 98


class Names:
    def __init__(self):
        self.ids = {}

    def __call__(self, *key):
        return self.ids.setdefault(key, len(self.ids))


def block_of(tiles):
    for a in range(1, 5):
        for b in range(1, 5):
            for r in range(1, 17):
                if tiles % (a * b * r) == 0 and tiles // (a * b * r) <= 16:
                    return a, b, r * 8, tiles // (a * b * r) * 128
    raise ValueError(tiles)


def kernel(NX, NY, NZ, NC, scale_ref, img_ref, txt_ref, dimg_ref, dtxt_ref, scal_ref,
           iall, tall, imgt, ee, gb, rsum, rel, csum, cel, rall, call_, uref, vref, ub, sc1, sc2,
           recv1, recv2, prt, zrecv, lead, ssem, rsem, lsem):
    D = img_ref.shape[1]
    NI, NT = NX * NY, NZ * NC
    XY, ZC = NI > 1, NT > 1
    H, Q = D // 2, D // 4
    inv = 1.0 / (2.0 * W * NI * NT)
    row, col = lax.axis_index("row"), lax.axis_index("col")
    x, c = lax.div(row, NC), lax.rem(row, NC)
    z, y = lax.div(col, NY), lax.rem(col, NY)
    mxy, mzc = x * NY + y, z * NC + c
    scale = scale_ref[0, 0]
    scale2 = scale * LOG2E
    rx = lambda v: lax.rem(v + 2 * NX, NX)
    ry = lambda v: lax.rem(v + 2 * NY, NY)
    rz = lambda v: lax.rem(v + 2 * NZ, NZ)

    def dev(px, py, pz, pc):
        return (pz * NY + py, px * NC + pc)

    plane = [(p, rx(x + p // NY), ry(y + p % NY)) for p in range(1, NI)]
    line = [(p, rz(z + p // NC), lax.rem(c + p % NC, NC)) for p in range(1, NT)]
    near_x, near_z = (lambda k: min(k, NX - k)), (lambda k: min(k, NZ - k))
    plane.sort(key=lambda p: -near_x(p[0] // NY) - near_x(p[0] % NY))
    line.sort(key=lambda p: -near_z(p[0] // NC) * NC - p[0] % NC)
    barrier = pltpu.get_barrier_semaphore()
    greet = []
    if XY:
        greet += [dev(rx(x + k), y, z, c) for k in (1, -1)] + [dev(x, ry(y + k), z, c) for k in (1, -1)]
    if ZC:
        greet += [dev(x, y, rz(z + k), c) for k in (1, -1)] + [dev(x, y, z, 1 - c)]
    for device in greet:
        pl.semaphore_signal(barrier, inc=1, device_id=device, device_id_type=MESH)
    loads = [pltpu.make_async_copy(img_ref, iall.at[x, y], lsem.at[0]), pltpu.make_async_copy(txt_ref, tall.at[z, c], lsem.at[1])]
    for load in loads:
        load.start()
    for ref in (csum, cel, rsum, rel, sc1, sc2):
        ref[...] = jnp.zeros_like(ref)
    with jax.named_scope("barrier"):
        for load in loads:
            load.wait()
        pl.semaphore_wait(barrier, len(greet))

    rid, sid = Names(), Names()
    sent = {}
    times = [1]

    def send(src, dst, key, device, group, offset=0):
        pltpu.make_async_remote_copy(
            src_ref=src, dst_ref=dst, send_sem=ssem.at[sid(group)], recv_sem=rsem.at[rid(*key) + offset],
            device_id=device, device_id_type=MESH).start()
        size = jnp.dtype(src.dtype).itemsize
        for n in src.shape:
            size *= n
        sent[group] = sent.get(group, 0) + size * times[0]

    def got(dst, key):
        pltpu.make_async_remote_copy(
            src_ref=dst, dst_ref=dst, send_sem=ssem.at[0], recv_sem=rsem.at[rid(*key)],
            device_id=dev(x, y, z, c), device_id_type=MESH).wait_recv()

    sg = (1, -1)
    lo, full = W // 4, W // 2

    def rows(half, part=None):
        start, size = half * full, full
        if part is not None:
            start, size = start + part * lo, lo
        return pl.ds(start, size)

    def first_dev(half, d):
        return dev(rx(x + sg[d]), y, z, c) if half == 0 else dev(x, ry(y + sg[d]), z, c)

    def second_dev(half, d):
        return dev(x, ry(y + sg[d]), z, c) if half == 0 else dev(rx(x + sg[d]), y, z, c)

    def first_piece(half, off):
        return (rx(x + off), y) if half == 0 else (x, ry(y + off))

    def second_piece(half, off1, off2):
        return (rx(x + off1), ry(y + off2)) if half == 0 else (rx(x + off2), ry(y + off1))

    def ipc(pc, sl):
        return iall.at[pc[0], pc[1], sl]

    def got_images(shards, key):
        got(iall.at[0, pl.ds(0, shards)], key)

    def got_texts(shards, key):
        got(tall.at[pl.ds(0, shards), 0], key)

    def first_send(half, d, t):
        if t == 1:
            ref = ipc((x, y), rows(half))
            send(ref, ref, ("f", d), first_dev(half, d), "f1")
        else:
            ref = ipc(first_piece(half, -sg[d]), rows(half, d))
            send(ref, ref, ("f2",), first_dev(half, d), "f2")

    def second_send(half, off, d, t):
        if t == 1:
            ref = ipc(second_piece(half, off, 0), rows(half))
            send(ref, ref, ("s", abs(off), d), second_dev(half, d), "s1")
        else:
            ref = ipc(second_piece(half, off, -sg[d]), rows(half, d))
            send(ref, ref, ("s2", off == 0), second_dev(half, d), "s2")

    def t_send(d, t, h):
        ref = tall.at[rz(z - sg[d] * (t - 1)), c, rows(h)]
        send(ref, ref, ("t", t, h if t < 4 else 0), dev(x, y, rz(z + sg[d]), c), "t")

    def t_pass(off, *part):
        if ZC:
            ref = tall.at[rz(z + off), c]
            ref = ref.at[rows(*part)] if part else ref
            send(ref, ref, ("p", max(abs(off), 1)), dev(x, y, z, 1 - c), "p")

    def t_passed(off):
        if ZC:
            got_texts((3, 2, 2, 1)[off - 1], ("p", off))

    both = (0, 1)

    def t_half(t, h):
        if ZC:
            with jax.named_scope(f"T{t}{h}"):
                got_texts(1, ("t", t, h))
            for d in both:
                if t < 3 or h == d:
                    t_send(d, t + 1, h)
            t_pass(-t, h)
            t_pass(t, h)

    def s_round(off):
        if XY:
            for d in both:
                got_images(2 if off == 1 else 1, ("s", off, d))
                for half in both:
                    for o in ((-1, 1) if off == 1 else (off,)):
                        second_send(half, o, d, 2)

    CW = NC * W

    def logits(shards, zs):
        lhs = jnp.concatenate([iall[i, j] for i, j in shards], axis=0)
        parts = [None, None]
        for zz in zs:
            cols = pl.ds(pl.multiple_of(zz * CW, W), CW)
            rhs = tall[zz].reshape(CW, D)
            dots = lax.dot_general(lhs, rhs, (((1,), (1,)), ((), ())), preferred_element_type=F32)
            lg = dots * scale2
            e = jnp.exp2(lg)
            el = e * lg
            for n, (i, j) in enumerate(shards):
                ee[i, j, :, cols] = e[n * W:(n + 1) * W]
            for m, (ref, val) in enumerate(((csum, e), (cel, el))):
                for k in range(NC):
                    part = val[:, k * W:(k + 1) * W]
                    parts[m] = part if parts[m] is None else parts[m] + part
                ref[:, cols] += jnp.sum(val.reshape(len(shards) * W // 8, 8, CW), axis=0)
        for ref, part in ((rsum, parts[0]), (rel, parts[1])):
            for n, (i, j) in enumerate(shards):
                ref[i, j] += part[n * W:(n + 1) * W]

    cross = [(x, y)]
    corners, across = [], []
    if XY:
        cross += [(rx(x - 1), y), (rx(x + 1), y), (x, ry(y - 1)), (x, ry(y + 1))]
        corners = [(rx(x + i), ry(y + j)) for i in (-1, 1) for j in (-1, 1)]
        across = [(x, ry(y + 2)), (rx(x + 2), y)]

    def tiles(name, shards, *offs):
        zs = [rz(z + off) for off in offs] if ZC else [z] if 0 in offs else []
        if shards and zs:
            with jax.named_scope(name):
                logits(shards, zs)

    def near(name, *offs):
        zs = [rz(z + off) for off in offs]

        def body(g, carry):
            i = rx(x + g - 1)
            logits([(i, ry(y - 1)), (i, y), (i, ry(y + 1))], zs)
            return carry

        with jax.named_scope(name):
            if ZC and XY:
                lax.fori_loop(0, 3, body, 0)
            elif ZC:
                logits(cross, zs)

    def whole(name, off):
        def body(i, carry):
            logits([(i, j) for j in range(NY)], [rz(z + off)])
            return carry

        with jax.named_scope(name):
            if ZC:
                lax.fori_loop(0, NX, body, 0)

    def far(name, pairs):
        with jax.named_scope(name):
            if not XY:
                return
            shards = [(rx(x - 1), ry(y + 2)), (rx(x + 1), ry(y + 2))] + [(rx(x + 2), ry(y + k)) for k in (-1, 1, 2)]

            def body(p, carry):
                logits(shards, [rz(z - p), rz(z + p)])
                return carry

            if not pairs:
                logits(shards, [z])
            elif ZC:
                lax.fori_loop(1, 4, body, 0)

    if XY:
        for half in both:
            for d in both:
                first_send(half, d, 1)
    if ZC:
        for h in both:
            for d in both:
                t_send(d, 1, h)
        t_pass(0)
    if XY:
        for half in both:
            for d in both:
                second_send(half, 0, d, 1)
        with jax.named_scope("f1"):
            for d in both:
                got_images(1, ("f", d))
                for half in both:
                    first_send(half, d, 2)
        for d in both:
            for half in both:
                for e in both:
                    second_send(half, -sg[d], e, 1)
    t_half(1, 0)
    t_half(1, 1)
    with jax.named_scope("s0"):
        s_round(0)
    if XY:
        with jax.named_scope("f2"):
            got_images(1, ("f2",))
        for half in both:
            for d in both:
                second_send(half, 2, d, 1)
    with jax.named_scope("p1"):
        t_passed(1)
    t_half(2, 0)
    tiles("C0", cross, -1, 0, 1)
    t_half(2, 1)
    with jax.named_scope("s1"):
        s_round(1)
    tiles("C1", corners, -1, 0, 1)
    t_half(3, 0)
    with jax.named_scope("p2"):
        t_passed(2)
    near("C2", -2, 2)
    t_half(3, 1)
    with jax.named_scope("s2"):
        s_round(2)
    with jax.named_scope("s0t2"):
        if XY:
            got_images(1, ("s2", True))
    tiles("C3", across, -2, -1, 0, 1, 2)
    with jax.named_scope("p3"):
        t_passed(3)
    near("C4", -3, 3)
    tiles("C4b", across, -3, 3)
    with jax.named_scope("end"):
        if XY:
            got_images(3, ("s2", False))
    far("C7", 0)
    with jax.named_scope("T4"):
        if ZC:
            got_texts(1, ("t", 4, 0))
            t_pass(4)
    far("C6", 1)
    with jax.named_scope("p4"):
        t_passed(4)
    whole("C5", 4)

    def share(buf, key, peers, me, to, rows=None):
        ref = buf.at[me] if rows is None else buf.at[me, pl.ds(0, rows)]
        for p in peers:
            send(ref, ref, (key,), to(p), key)

    def shared(buf, key, peers, rows=None):
        if peers:
            ref = buf.at[pl.ds(0, len(peers))]
            got(ref if rows is None else ref.at[:, pl.ds(0, rows)], (key,))
        total = buf[0]
        for k in range(1, len(peers) + 1):
            total = total + buf[k]
        return total

    to_plane = lambda p: dev(p[1], p[2], z, c)
    to_line = lambda p: dev(x, y, p[1], p[2])
    for k in range(NT):
        call_[mzc, k:k + 1, :] = jnp.sum(csum[:, k * W:(k + 1) * W], axis=0, keepdims=True)
    share(call_, "c", line, mzc, to_line)
    for k in range(NI):
        rall[mxy, k:k + 1, :] = jnp.sum(jnp.transpose(rsum[k // NY, k % NY]), axis=0, keepdims=True)
    share(rall, "r", plane, mxy, to_plane)
    with jax.named_scope("imgt"):
        for k in range(NI):
            tr = jnp.transpose(iall[k // NY, k % NY])
            for d in both:
                imgt[d, :, k * W:(k + 1) * W] = tr[d * H:(d + 1) * H]
        prod = iall[x, y].astype(F32) * tall[z, c].astype(F32)
        pos = prod[:, :W]
        for k in range(1, D // W):
            pos = pos + prod[:, k * W:(k + 1) * W]
        pos = scale * jnp.sum(pos, axis=0, keepdims=True)
    with jax.named_scope("rwait"):
        rtot = shared(rall, "r", plane)
    u = inv / rtot
    for k in range(NI):
        ub[k // NY, k % NY] = jnp.transpose(jnp.broadcast_to(u[k:k + 1, :], (W, W)))
    with jax.named_scope("cwait"):
        ctot = shared(call_, "c", line)
    v = inv / ctot
    uref[...] = rtot
    vref[...] = v

    def build(i, j):
        uu = ub[i, j]
        for k in range(NT):
            sl = slice(k * W, (k + 1) * W)
            gb[i, j, :, sl] = (ee[i, j, :, sl] * (uu + vref[k:k + 1, :])).astype(BF16)

    def builds(n, place):
        def body(k, carry):
            build(*place(k))
            return carry

        lax.fori_loop(0, n, body, 0)

    def unit_t(s):
        def body(d, carry):
            zz = rz(z - (1 - 2 * d) * (s + 1))
            rhs = gb[:, :, :, pl.ds(pl.multiple_of(zz * CW, W), CW)].reshape(NI * W, CW)
            res = jnp.dot(imgt[d], rhs, preferred_element_type=F32)
            for k in range(NC):
                ee[d * 2 + k, :, :, 1024 + s * W:1024 + (s + 1) * W] = res[:, k * W:(k + 1) * W].reshape(4, W, W)
            send(ee.at[d * 2 + 1 - c, :, :, pl.ds(1024 + s * W, W)], prt.at[d, s], ("w", s), dev(x, y, z, 1 - c), "w")
            return carry

        with jax.named_scope(f"ut{s}"):
            times[0] = 2
            lax.fori_loop(0, 2, body, 0)
            times[0] = 1

    def unit_i1(first, d, j):
        q = first * 2 + d
        step = (1 - 2 * d) * (j + 1)
        lhs = gb[:, ry(y - step)] if first == 0 else gb[rx(x - step)]
        rhs = tall[:, :, :, pl.ds(pl.multiple_of(q * Q, W), Q)].reshape(NT * W, Q)
        res = jnp.dot(lhs.reshape(4 * W, NT * W), rhs, preferred_element_type=F32)
        if j == 0:
            lead[q] = res.reshape(4, W, Q)
        else:
            ee[q, :, :, j * Q:(j + 1) * Q] = res.reshape(4, W, Q)

    def unit_i(first, j):
        def body(d, carry):
            unit_i1(first, d, j)
            return carry

        with jax.named_scope(f"ui{first}{j}"):
            lax.fori_loop(0, 2, body, 0)

    def i_dev(q, along_y, sign):
        return dev(x, ry(y + sign), z, c) if along_y else dev(rx(x + sign), y, z, c)

    def i_place(q, k):
        off = (2, sg[q % 2], -sg[q % 2], 0)[k]
        return rx(x + off) if q < 2 else ry(y + off)

    def i_step(d, j, k):
        got(recv1.at[0, 0, pl.ds(0, 2)], ("i", d, j - 1, k))
        for q in (d, d + 2):
            at, sign = i_place(q, k), sg[d]
            here = recv1.at[q, j - 1, at]
            here[...] += ee[q, at, :, j * Q:(j + 1) * Q]
            if j < 3:
                send(here, recv1.at[q, j, at], ("i", d, j, k), i_dev(q, q < 2, sign), "i")
            elif k == 0:
                send(here, recv2.at[q, 0], ("j", q, 0), i_dev(q, q >= 2, sign), "j")
            elif k == 2:
                send(here, recv2.at[q, 2], ("j", q, 2), i_dev(q, q >= 2, -sign), "j")

    def i_pass(q):
        here = recv2.at[q, 0]
        got(here, ("j", q, 0))
        here[...] += recv1[q, 2, i_place(q, 1)]
        send(here, recv2.at[q, 1], ("j", q, 1), i_dev(q, q >= 2, sg[q % 2]), "j")

    def i_last(q):
        got(recv2.at[q, 2], ("j", q, 2))
        got(recv2.at[q, 1], ("j", q, 1))
        block = recv1[q, 2, i_place(q, 3)] + recv2[q, 2] + recv2[q, 1]
        dimg_ref[:, q * Q:(q + 1) * Q] = (block * scale).astype(BF16)

    def z_step(s, k):
        if k == 0:
            got(prt.at[:, s], ("w", s))
        if s > 0:
            got(zrecv.at[:, s - 1, k], ("z", s - 1, k))
        for d in both:
            mine = ee.at[d * 2 + c, k, :, pl.ds(1024 + s * W, W)]
            if s == 0:
                mine[...] += prt[d, s, k]
                here = mine
            else:
                here = zrecv.at[d, s - 1, k]
            if s == 7:
                w = d * 4 + k
                block = here[...] + (mine[...] + prt[d, s, k])
                dtxt_ref[:, w * W:(w + 1) * W] = (jnp.transpose(block) * scale).astype(BF16)
                continue
            if s > 0:
                here[...] += mine[...] + prt[d, s, k]
            send(here, zrecv.at[d, s, k], ("z", s, k), dev(x, y, rz(z + sg[d]), c), "z")

    def totals():
        dts = jnp.zeros((8, W), F32)
        for k in range(NT):
            dts = dts + cel[:, k * W:(k + 1) * W] * vref[k:k + 1, :]

        def body(i, acc):
            for j in range(NY):
                acc = acc + jnp.sum((ub[i, j] * rel[i, j]).reshape(W // 8, 8, W), axis=0)
            return acc

        dts = lax.fori_loop(0, NX, body, dts)
        dt_part = jnp.sum(dts, axis=0, keepdims=True) * (1.0 / LOG2E) - (2.0 * inv) * pos
        loss = jnp.log(uref[pl.ds(mxy, 1), :]) - jnp.log(vref[pl.ds(mzc, 1), :] * (1.0 / inv)) - 2.0 * pos
        line_no = lax.broadcasted_iota(jnp.int32, (8, W), 0)
        sc1[mxy] = jnp.where(line_no == 0, jnp.broadcast_to(loss * inv, (8, W)),
                             jnp.where(line_no == 1, jnp.broadcast_to(dt_part, (8, W)), 0.0))
        share(sc1, "m", plane, mxy, to_plane, 2)

    def totals2():
        sc2[mzc] = shared(sc1, "m", plane, 2)
        share(sc2, "n", line, mzc, to_line, 2)

    def start(d):
        sign = sg[d]
        builds(4 - d, lambda k: (rx(x + k), ry(y - sign)))
        builds(3 - d, lambda k: (rx(x - sign), ry(y + k * (1 + d))))

    def start_send(d):
        for first in both:
            unit_i1(first, d, 0)
        for k in range(4):
            for q in (d, d + 2):
                place = i_place(q, k)
                send(lead.at[q, place], recv1.at[q, 0, place], ("i", d, 0, k), i_dev(q, q < 2, sg[d]), "i")

    if XY:
        with jax.named_scope("start0"):
            start(0)
            start_send(0)
        with jax.named_scope("start1"):
            start(1)
            start_send(1)
            builds(4, lambda k: (rx(x + 2 * lax.div(k, 2)), ry(y + 2 * lax.rem(k, 2))))
    else:
        build(0, 0)
    own = pl.ds(pl.multiple_of(mzc * W, W), W)
    eye = lax.broadcasted_iota(jnp.int32, (W, W), 0) == lax.broadcasted_iota(jnp.int32, (W, W), 1)
    gb[x, y, :, own] = (ee[x, y, :, own] * (ub[x, y] + vref[pl.ds(mzc, 1), :])
                        - jnp.where(eye, 2.0 * inv, 0.0)).astype(BF16)
    STEP, SUB, Z0 = 5.65, 2.82, 5.6
    base = (0.0, 2.0)
    events = []

    def at(time, fn, *args):
        events.append((time, len(events), fn, args))

    def z_time(s, k):
        return Z0 + (s - 1) * STEP + 1.7 + SUB / 2 * (k + 1) if s else Z0

    if ZC:
        for s, slot in ((0, 0.0), (1, 4.5), (2, Z0 + 0.05), (3, z_time(1, 3)), (4, z_time(2, 3)), (5, z_time(4, 1)),
                        (6, z_time(4, 3)), (7, z_time(5, 1))):
            at(slot + 0.01, unit_t, s)
        for s in range(8):
            for k in range(4):
                at(z_time(s, k), z_step, s, k)
    if XY:
        for first, slots in ((0, (Z0, z_time(1, 1), z_time(3, 1))), (1, (Z0, z_time(2, 1), z_time(3, 3)))):
            for j in range(1, 4):
                at(slots[j - 1] + 0.02, unit_i, first, j)
        for d in both:
            for j in range(1, 4):
                for k in range(4):
                    wait = (base[d] + 1.7 + (j - 1) * 2 * STEP + (k + 1) * SUB + (1.8, 2.0, 0.8)[j - 1])
                    at(max(wait, Z0 + 0.03) if j == 1 else wait, i_step, d, j, k)
            for q in (d, d + 2):
                at(base[d] + 38.5, i_pass, q)
                at(base[d] + 44.0, i_last, q)
    at(z_time(1, 1) + 0.015, totals)
    at(25.0, totals2)
    for _, _, fn, args in sorted(events, key=lambda e: e[:2]):
        with jax.named_scope("_".join([fn.__name__] + [str(v) for v in args])):
            fn(*args)

    with jax.named_scope("fin"):
        total = shared(sc2, "n", line, 2)
        scal_ref[...] = jnp.broadcast_to(jnp.sum(total, axis=1, keepdims=True), (8, W))
    for group, size in sent.items():
        if group in ("m", "n"):
            ref = (sc1 if group == "m" else sc2).at[pl.ds(0, size // 1024), pl.ds(0, 2)]
            pltpu.make_async_remote_copy(
                src_ref=ref, dst_ref=ref, send_sem=ssem.at[sid(group)], recv_sem=rsem.at[0],
                device_id=dev(x, y, z, c), device_id_type=MESH).wait_send()
            continue
        a, b, r, l = block_of(size // 4096)
        ref = ee.at[pl.ds(0, a), pl.ds(0, b), pl.ds(0, r), pl.ds(0, l)]
        pltpu.make_async_remote_copy(
            src_ref=ref, dst_ref=ref, send_sem=ssem.at[sid(group)], recv_sem=rsem.at[0],
            device_id=dev(x, y, z, c), device_id_type=MESH).wait_send()
    assert len(sid.ids) <= N_SEND and len(rid.ids) <= N_RECV, (len(sid.ids), len(rid.ids))

def call(NX, NY, NZ, NC, scale, img, txt):
    D = img.shape[1]
    NI, NT = NX * NY, NZ * NC
    H, Q = D // 2, D // 4
    vmem = pltpu.VMEM
    return pl.pallas_call(
        functools.partial(kernel, NX, NY, NZ, NC),
        out_shape=(jax.ShapeDtypeStruct(img.shape, BF16), jax.ShapeDtypeStruct(txt.shape, BF16),
                   jax.ShapeDtypeStruct((8, W), F32)),
        in_specs=[pl.BlockSpec(memory_space=pltpu.SMEM)] + [pl.BlockSpec(memory_space=pl.ANY)] * 2,
        out_specs=[pl.BlockSpec(memory_space=vmem)] * 3,
        scratch_shapes=[
            vmem((NX, NY, W, D), BF16), vmem((NZ, NC, W, D), BF16), vmem((2, H, NI * W), BF16),
            vmem((4, 4, W, 2048), F32), vmem((NX, NY, W, NT * W), BF16),
            vmem((NX, NY, W, W), F32), vmem((NX, NY, W, W), F32), vmem((8, NT * W), F32), vmem((8, NT * W), F32),
            vmem((NI, NI, W), F32), vmem((NT, NT, W), F32), vmem((NI, W), F32), vmem((NT, W), F32),
            vmem((NX, NY, W, W), F32), vmem((NI, 8, W), F32), vmem((NT, 8, W), F32),
            vmem((4, 3, 4, W, Q), F32), vmem((4, 3, W, Q), F32),
            vmem((2, 8, 4, W, W), F32), vmem((2, 7, 4, W, W), F32), vmem((4, 4, W, Q), F32),
            pltpu.SemaphoreType.DMA((N_SEND,)), pltpu.SemaphoreType.DMA((N_RECV,)),
            pltpu.SemaphoreType.DMA((2,)),
        ],
        compiler_params=pltpu.CompilerParams(collective_id=0, has_side_effects=True, vmem_limit_bytes=67043328),
    )(scale, img, txt)


def finish(img_ref, txt_ref, scal_ref, dimg_ref, dtxt_ref, loss_ref, dt_ref):
    dimg_ref[...] = img_ref[...]
    dtxt_ref[...] = txt_ref[...]
    loss_ref[0, 0] = scal_ref[0, 0]
    dt_ref[0, 0] = scal_ref[1, 0]


SHAPE = (4, 4, 8, 2)


def solution(mesh):
    batch_spec = P(("row", "col"), None)

    def local_tile(img_loc, txt_loc, log_scale):
        scale = jnp.exp(log_scale).reshape(1, 1)
        d_img, d_txt, scal = call(*SHAPE, scale, img_loc, txt_loc)
        vmem = pl.BlockSpec(memory_space=pltpu.VMEM)
        smem = pl.BlockSpec(memory_space=pltpu.SMEM)
        one = jax.ShapeDtypeStruct((1, 1), F32)
        d_img, d_txt, loss, d_scale = pl.pallas_call(
            finish, out_shape=(jax.ShapeDtypeStruct(d_img.shape, BF16), jax.ShapeDtypeStruct(d_txt.shape, BF16), one, one),
            in_specs=[vmem, vmem, smem], out_specs=[vmem, vmem, smem, smem])(d_img, d_txt, scal)
        return loss[0, 0], d_img, d_txt, d_scale[0, 0]

    return jax.shard_map(local_tile, mesh=mesh, in_specs=(batch_spec, batch_spec, P()),
                         out_specs=(P(), batch_spec, batch_spec, P()), check_vma=False)
```
